32 devices in a mesh: gx: 8 (over y, x, core), wa: 4 (over z).
Axes of the slice: x: 2, y: 2, z: 4, core: 2. Of those that a mesh axis runs over, the one named last changes fastest.
Arguments:
- warm_field: float32 [64, 2, 128, 2048], P('wa', None, 'gx'), may hold values from -1.8 to 1.8
- warm_adjoint: float32 [64, 2, 128, 2048], P('wa', None, 'gx'), may hold values from -1.8 to 1.8
- permittivity: float32 [128, 2048], P('gx'), may hold values from 1 to 12
- design_mask: int32 [128, 2048], P('gx'), may hold values 0 or 1
- source_row: int32 [64], P('wa'), may hold values from 0 to 127
- monitor_row: int32 [64], P('wa'), may hold values from 0 to 127
- wavenumber: float32 [64], P('wa'), may hold values from 0.02 to 0.08
- bloch_phase: float32 [64], P('wa'), may hold values from -3.140625 to 3.140625
- source_profile: float32 [64, 2, 2048], P('wa'), may hold values from -24 to 24
- monitor_profile: float32 [64, 2, 2048], P('wa'), may hold values from -4 to 4
Outputs:
- forward_field: float32 [64, 2, 128, 2048], P('wa', None, 'gx')
- adjoint_field: float32 [64, 2, 128, 2048], P('wa', None, 'gx')
- gradient: float32 [128, 2048], P('gx')
The draws below stay inside these ranges and needn't reach their ends.
All inputs are finite; a program needn't handle non-finite values. No bound on the sum of `design_mask` on one device may be relied on, other than what follows from the above.
Results may differ from the reference program's by a relative error of at most 0.0003.
Values sent between devices are 32-bit elements; how exact they have to be, the bound alone decides.
A program may use at most 128 MiB of HBM per device.

```python
import math
import jax
import jax.numpy as jnp
from jax import lax

NY = 2048
NX = 128
WAVES = 64


rough_amp = 0.01


smooth_amp = 0.3


noise_share = 0.005


def wave_kinds(key):
    ranking = jax.random.permutation(jax.random.fold_in(key, 5), WAVES)
    return ranking < max(1, WAVES // 4)


def rough_start(key):
    key_base, key_rows, key_cols = jax.random.split(key, 3)
    position = jnp.arange(NX, dtype=jnp.float32) / NX
    jitter = jax.random.uniform(key_rows, (NX,), jnp.float32, -0.15, 0.15)
    row_scale = jnp.exp(math.log(10.0) * jnp.clip(position + jitter, 0.0, 1.0))
    col_scale = jnp.exp(jax.random.uniform(key_cols, (NY,), jnp.float32, 0.0, math.log(3.0)))
    texture = jnp.clip(jax.random.normal(key_base, (WAVES, 2, NX, NY), jnp.float32), -6.0, 6.0)
    return rough_amp * texture * row_scale[:, None] * col_scale


def smooth_start(key):
    key_rotation, key_rough = jax.random.split(key)
    along_x = jnp.sin(math.pi * (jnp.arange(NX, dtype=jnp.float32) + 0.5) / NX)
    along_y = jnp.sin(math.pi * (jnp.arange(NY, dtype=jnp.float32) + 1.0) / (NY + 1))
    rotation = jax.random.uniform(key_rotation, (WAVES,), jnp.float32, -math.pi, math.pi)
    phasor = jnp.stack([jnp.cos(rotation), jnp.sin(rotation)], axis=1)
    envelope = along_x[:, None] * along_y[None, :]
    roughness = jnp.clip(jax.random.normal(key_rough, (WAVES, 2, NX, NY), jnp.float32), -6.0, 6.0)
    return smooth_amp * (phasor[:, :, None, None] * envelope + noise_share * roughness)


def blended_start(key, stream_salt):
    own_key = jax.random.fold_in(key, stream_salt)
    smooth_kind = wave_kinds(key)
    return jnp.where(smooth_kind[:, None, None, None], smooth_start(jax.random.fold_in(own_key, 1)), rough_start(jax.random.fold_in(own_key, 2)))


def profile_draw(key, stream_salt, scale, bound, weak):
    own_key = jax.random.fold_in(key, stream_salt)
    smooth_kind = wave_kinds(key)
    texture = jnp.clip(jax.random.normal(own_key, (WAVES, 2, NY), jnp.float32), -bound, bound)
    weight = jnp.where(smooth_kind, weak, 1.0)
    return scale * weight[:, None, None] * texture


def draw_warm_field(key, part):
    return blended_start(key, 11)


def draw_warm_adjoint(key, part):
    return blended_start(key, 23)


def draw_source_profile(key, part):
    return profile_draw(key, 31, 4.0, 6.0, 0.004)


def draw_monitor_profile(key, part):
    return profile_draw(key, 37, 1.0, 4.0, 0.02)


def place_ends(result, rng, least, top_value):
    shape = result.shape
    place = [jax.random.randint(jax.random.fold_in(rng, axis), (), 0, shape[axis]) for axis in range(len(shape))]
    result = result.at[tuple(place)].set(least)
    longest = shape.index(max(shape))
    place[longest] = (place[longest] + 1) % shape[longest]
    return result.at[tuple(place)].set(top_value)


def shard_levels(key, dims, shards, smallest, top_value):
    gain = 1.0
    for dim, parts in shards:
        heights = jax.random.uniform(jax.random.fold_in(jax.random.fold_in(key, 6), dim), (parts,), jnp.float32, smallest / len(shards), top_value / len(shards))
        gain = gain * jnp.repeat(jnp.exp(heights), dims[dim] // parts).reshape((-1,) + (1,) * (len(dims) - 1 - dim))
    return gain


def setup_inputs(seed: int = 0) -> dict:
    key_list = jax.random.split(jax.random.key(seed), 11)
    warm_field = draw_warm_field(jax.random.fold_in(key_list[10], 71), 0)
    warm_adjoint = draw_warm_adjoint(jax.random.fold_in(key_list[10], 71), 0)
    permittivity = jnp.clip(1.0 + 11.0 * jax.random.uniform(key_list[2], (NX, NY), jnp.float32) ** shard_levels(key_list[2], (NX, NY), ((0, 8),), -0.2, 0.2), 1.0, 12.0)
    design_mask = place_ends((jax.random.randint(key_list[3], (NX, NY), 0, 2) < 1).astype(jnp.int32), jax.random.fold_in(key_list[3], 1), 0, 1)
    source_row = place_ends(jax.random.randint(key_list[4], (WAVES,), 0, NX), jax.random.fold_in(key_list[4], 1), 0, NX - 1).astype(jnp.int32)
    monitor_row = place_ends(jax.random.randint(key_list[5], (WAVES,), 0, NX), jax.random.fold_in(key_list[5], 1), 0, NX - 1).astype(jnp.int32)
    wavenumber = jnp.clip(jnp.exp(math.log(0.08) - 1.3862944 * jax.random.uniform(key_list[6], (WAVES,), jnp.float32) ** shard_levels(key_list[6], (WAVES,), ((0, 4),), -0.2, 0.2)), 0.02, 0.08)
    bloch_phase = jnp.clip(jax.random.uniform(key_list[7], (WAVES,), jnp.float32, -3.140625, 3.140625), -3.140625, 3.140625)
    source_profile = draw_source_profile(jax.random.fold_in(key_list[10], 71), 0)
    monitor_profile = draw_monitor_profile(jax.random.fold_in(key_list[10], 71), 0)
    return dict(warm_field=warm_field, warm_adjoint=warm_adjoint, permittivity=permittivity, design_mask=design_mask, source_row=source_row, monitor_row=monitor_row, wavenumber=wavenumber, bloch_phase=bloch_phase, source_profile=source_profile, monitor_profile=monitor_profile)


floor_share = 0.5


def rotate(part, cosine, sine):
    return jnp.stack([cosine * part[0] - sine * part[1], sine * part[0] + cosine * part[1]])


def operate(field, diagonal, cosine, sine):
    above = jnp.concatenate([field[:, 1:], rotate(field[:, :1], cosine, sine)], axis=1)
    below = jnp.concatenate([rotate(field[:, -1:], cosine, -sine), field[:, :-1]], axis=1)
    zero_col = jnp.zeros_like(field[..., :1])
    y_after = jnp.concatenate([field[..., 1:], zero_col], axis=-1)
    y_before = jnp.concatenate([zero_col, field[..., :-1]], axis=-1)
    return diagonal * field - (above + below + y_after + y_before)


def complex_scale(scale_re, scale_im, vector):
    return jnp.stack([scale_re * vector[0] - scale_im * vector[1], scale_re * vector[1] + scale_im * vector[0]])


def solve_step(right_side, initial, diagonal, cosine, sine):
    residual = right_side - operate(initial, diagonal, cosine, sine)
    res_norm = jnp.sum(residual * residual)
    precond = residual / diagonal
    image = operate(precond, diagonal, cosine, sine)
    dot_re = jnp.sum(residual[0] * image[0] + residual[1] * image[1])
    dot_im = jnp.sum(residual[0] * image[1] - residual[1] * image[0])
    bounded = jnp.maximum(dot_re * dot_re + dot_im * dot_im, (floor_share * res_norm) * (floor_share * res_norm))
    step_re = res_norm * dot_re / bounded
    step_im = -res_norm * dot_im / bounded
    shrunk = residual - complex_scale(step_re, step_im, image)
    second = shrunk / diagonal
    turned = operate(second, diagonal, cosine, sine)
    ts_re = jnp.sum(turned[0] * shrunk[0] + turned[1] * shrunk[1])
    ts_im = jnp.sum(turned[0] * shrunk[1] - turned[1] * shrunk[0])
    tt_sum = jnp.sum(turned * turned)
    omega_re = ts_re / tt_sum
    omega_im = ts_im / tt_sum
    return initial + complex_scale(step_re, step_im, precond) + complex_scale(omega_re, omega_im, second)


def reference(warm_field, warm_adjoint, permittivity, design_mask, source_row, monitor_row, wavenumber, bloch_phase, source_profile, monitor_profile):
    row_index = jnp.arange(NX)

    def per_wave(running, packed):
        start_fwd, start_adj, src_at, mon_at, squared_k, phase_angle, src_prof, mon_prof = packed
        diagonal = 4.0 - squared_k * permittivity
        cosine = jnp.cos(phase_angle)
        sine = jnp.sin(phase_angle)
        src_sel = (row_index == src_at).astype(jnp.float32)[None, :, None]
        right_side = src_sel * src_prof[:, None, :]
        forward = solve_step(right_side, start_fwd, diagonal, cosine, sine)
        mon_sel = (row_index == mon_at).astype(jnp.float32)
        mon_vals = jnp.sum(mon_sel[None, :, None] * forward, axis=1)
        over_re = jnp.sum(mon_prof[0] * mon_vals[0] + mon_prof[1] * mon_vals[1])
        over_im = jnp.sum(mon_prof[0] * mon_vals[1] - mon_prof[1] * mon_vals[0])
        adj_re = over_re * mon_prof[0] - over_im * mon_prof[1]
        adj_im = -(over_re * mon_prof[1] + over_im * mon_prof[0])
        adj_side = mon_sel[None, :, None] * jnp.stack([adj_re, adj_im])[:, None, :]
        adjoint = solve_step(adj_side, start_adj, diagonal, cosine, -sine)
        contrib = 2.0 * squared_k * (adjoint[0] * forward[0] - adjoint[1] * forward[1])
        return running + contrib, (forward, adjoint)

    summed_init = jnp.zeros((NX, NY), jnp.float32)
    summed, outputs = lax.scan(per_wave, summed_init, (warm_field, warm_adjoint, source_row, monitor_row, wavenumber, bloch_phase, source_profile, monitor_profile))
    gradient = design_mask.astype(jnp.float32) * summed
    return outputs[0], outputs[1], gradient
```

```python
import functools

import jax
import jax.numpy as jnp
from jax import lax
from jax.experimental import pallas as pl
from jax.experimental.pallas import tpu as pltpu
from jax.sharding import PartitionSpec as P

floor_share = 0.5
REACH = 3
TILE = 8
LANES = 128
QUARTERS = 4
SUMS = 16
VMEM_LIMIT = 50000 * 1024


def col(tile):
    return slice(tile * LANES, (tile + 1) * LANES)


def sideways(load, tiles):
    tile = load(0)
    lane = lax.broadcasted_iota(jnp.int32, tile.shape, 1)
    at_right, at_left = lane == LANES - 1, lane == 0
    after, before = pltpu.roll(tile, LANES - 1, 1), pltpu.roll(tile, 1, 1)
    carried = jnp.zeros_like(tile)
    for ct in range(tiles):
        if ct + 1 < tiles:
            ahead = load(ct + 1)
            next_after, next_before = pltpu.roll(ahead, LANES - 1, 1), pltpu.roll(ahead, 1, 1)
        else:
            ahead, next_after, next_before = None, jnp.zeros_like(tile), None
        near = jnp.where(at_right, next_after, after) + jnp.where(at_left, carried, before)
        yield near
        carried, tile, after, before = before, ahead, next_after, next_before


def updown(tile):
    total = tile.shape[0]
    return pltpu.roll(tile, total - 1, 0) + pltpu.roll(tile, 1, 0)


def fold(cells):
    acc = cells[:TILE]
    for start in range(TILE, cells.shape[0], TILE):
        acc = acc + cells[start : start + TILE]
    return acc


def pair_products(a, b):
    return fold(a[0] * b[0] + a[1] * b[1]), fold(a[0] * b[1] - a[1] * b[0])


def times(a, b):
    return a[0] * b[0] - a[1] * b[1], a[0] * b[1] + a[1] * b[0]


def scalars_of(total, with_overlap):
    q = [total[:, i : i + 1] for i in range(SUMS)]
    res_norm, rv_re, rv_im, image_sq, wr_re, wr_im, wv_re, wv_im, twice_sq = q[:9]
    half = floor_share * res_norm
    bounded = jnp.maximum(rv_re * rv_re + rv_im * rv_im, half * half)
    step_re = res_norm * rv_re / bounded
    step_im = -res_norm * rv_im / bounded
    step_sq = step_re * step_re + step_im * step_im
    ts_re = rv_re - step_re * image_sq - (step_re * wr_re + step_im * wr_im) + step_sq * wv_re
    ts_im = -rv_im - step_im * image_sq - (step_re * wr_im - step_im * wr_re) + step_sq * wv_im
    tt_sum = image_sq - 2.0 * (step_re * wv_re + step_im * wv_im) + step_sq * twice_sq
    omega_re = ts_re / tt_sum
    omega_im = ts_im / tt_sum
    both_re, both_im = times((step_re, step_im), (omega_re, omega_im))
    found = [step_re + omega_re, step_im + omega_im, -both_re, -both_im]
    if with_overlap:
        mx_re, mx_im, mz_re, mz_im, my_re, my_im = q[9:15]
        for_z = times(found[0:2], (mz_re, mz_im))
        for_y = times(found[2:4], (my_re, my_im))
        found.append(mx_re + for_z[0] + for_y[0])
        found.append(mx_im + for_z[1] + for_y[1])
    return found


def step_kernel(
    count, depth,
    turns, wave_k, src_row, mon_row, eps_hbm, field_hbm, adjoint_hbm, mask_hbm, src_hbm, mon_hbm,
    fwd, adj, grad,
    ext, zed, yed, send, recv, res, img, diag, inverse, eps, eps_send, eps_recv, src, mon, mask,
    parts, mine, got, coef, gpart, ggot, gtotal, gspread,
    load_sem, side_sem, halo_sems, eps_sems, sum_sems, grad_sems,
):
    waves, _, rows, width = field_hbm.shape
    total = rows + TILE
    tiles = width // LANES
    quarter = width // QUARTERS
    whole = rows * count
    me = lax.axis_index("gx")
    level = lax.axis_index("wa")
    before, after = lax.rem(me - 1 + count, count), lax.rem(me + 1, count)
    at_first, at_last = me == 0, me == count - 1

    fields = (field_hbm, adjoint_hbm)

    def load(field, wave):
        return pltpu.make_async_copy(
            fields[field].at[wave], ext.at[field, wave, :, pl.ds(0, rows)],
            load_sem.at[field, wave],
        )

    sides = [
        pltpu.make_async_copy(eps_hbm, eps.at[pl.ds(0, rows)], side_sem.at[0]),
        pltpu.make_async_copy(src_hbm, src, side_sem.at[1]),
        pltpu.make_async_copy(mon_hbm, mon, side_sem.at[2]),
        pltpu.make_async_copy(mask_hbm, mask, side_sem.at[3]),
    ]
    sides[0].start()
    for wave in range(waves):
        load(0, wave).start()
    for copy in sides[1:]:
        copy.start()
    for wave in range(waves):
        load(1, wave).start()

    barrier = pltpu.get_barrier_semaphore()
    for axis, size, own in (("gx", count, me), ("wa", depth, level)):
        for hop in range(1, size):
            pl.semaphore_signal(
                barrier, inc=1, device_id={axis: lax.rem(own + hop, size)},
                device_id_type=pl.DeviceIdType.MESH,
            )

    sides[0].wait()
    for way, low in ((0, 0), (1, rows - REACH)):
        for part in range(QUARTERS):
            span = slice(part * quarter, (part + 1) * quarter)
            eps_send[way, part * 4 : part * 4 + REACH] = eps[low : low + REACH, span]

    def neighbour(way):
        return {"gx": before if way == 0 else after}

    def eps_move(way):
        return pltpu.make_async_remote_copy(
            src_ref=eps_send.at[way], dst_ref=eps_recv.at[way],
            send_sem=eps_sems.at[0, way], recv_sem=eps_sems.at[1, way],
            device_id=neighbour(way), device_id_type=pl.DeviceIdType.MESH,
        )

    def halo_move(field, way, wave):
        return pltpu.make_async_remote_copy(
            src_ref=send.at[field, way, wave], dst_ref=recv.at[field, way, wave],
            send_sem=halo_sems.at[0, field, way, wave],
            recv_sem=halo_sems.at[1, field, way, wave],
            device_id=neighbour(way), device_id_type=pl.DeviceIdType.MESH,
        )

    def pack(field, wave):
        for way, low in ((0, 0), (1, rows - REACH)):
            for c in range(2):
                for part in range(QUARTERS):
                    span = slice(part * quarter, (part + 1) * quarter)
                    at = part * 2 * REACH + c * REACH
                    send[field, way, wave, at : at + REACH] = ext[
                        field, wave, c, low : low + REACH, span
                    ]

    pl.semaphore_wait(barrier, count - 1 + depth - 1)
    for way in range(2):
        eps_move(way).start()

    def first_sends(wave, carry):
        load(0, wave).wait()
        pack(0, wave)
        for way in range(2):
            halo_move(0, way, wave).start()
        return carry

    lax.fori_loop(0, waves, first_sends, 0)
    for copy in sides[1:]:
        copy.wait()

    def adjoint_packs(wave, carry):
        load(1, wave).wait()
        pack(1, wave)
        return carry

    lax.fori_loop(0, waves, adjoint_packs, 0)

    for way, at in ((0, rows), (1, total - REACH)):
        eps_move(way).wait_recv()
        for part in range(QUARTERS):
            span = slice(part * quarter, (part + 1) * quarter)
            eps[at : at + REACH, span] = eps_recv[way, part * 4 : part * 4 + REACH]
    eps[rows + REACH : total - REACH] = jnp.ones((TILE - 2 * REACH, width), jnp.float32)

    row_of = lax.broadcasted_iota(jnp.int32, (total, LANES), 0)

    def spot_of(row):
        away = row - me * rows
        away = jnp.where(away < 0, away + whole, away)
        spot = jnp.where(
            away < rows + REACH, away,
            jnp.where(away >= whole - REACH, away - whole + total, -1),
        )
        return spot

    def turn_of(spot, wave, sign):
        cosine, sine = turns[0, wave], sign * turns[1, wave]
        above = (spot >= rows) & (spot < rows + REACH) & at_last
        below = (spot >= rows + REACH) & at_first
        turn_c = jnp.where(above | below, cosine, 1.0)
        turn_s = jnp.where(above, sine, jnp.where(below, -sine, 0.0))
        return turn_c, turn_s

    def unpack(field, wave, sign):
        cosine, sine = turns[0, wave], sign * turns[1, wave]
        for way, at in ((0, rows), (1, total - REACH)):
            edge = at_last if way == 0 else at_first
            turn_c = jnp.where(edge, cosine, 1.0)
            turn_s = jnp.where(edge, sine if way == 0 else -sine, 0.0)
            for part in range(QUARTERS):
                span = slice(part * quarter, (part + 1) * quarter)
                base = part * 2 * REACH
                got_re = recv[field, way, wave, base : base + REACH]
                got_im = recv[field, way, wave, base + REACH : base + 2 * REACH]
                ext[field, wave, 0, at : at + REACH, span] = turn_c * got_re - turn_s * got_im
                ext[field, wave, 1, at : at + REACH, span] = turn_s * got_re + turn_c * got_im

    def images(field, wave, spot, side_row, with_overlap):
        squared_k = wave_k[wave]
        for ct in range(tiles):
            d = 4.0 - squared_k * eps[:, col(ct)]
            diag[:, col(ct)] = d
            inverse[:, col(ct)] = 1.0 / d
        here = row_of == spot
        nears = [
            sideways(lambda ct, c=c: ext[field, wave, c, :, col(ct)], tiles) for c in range(2)
        ]
        for ct in range(tiles):
            rows_in = side_row(ct)
            for c in range(2):
                near = next(nears[c])
                x = ext[field, wave, c, :, col(ct)]
                r = (near + updown(x)) - diag[:, col(ct)] * x
                r = jnp.where(here, r + rows_in[c], r)
                res[c, :, col(ct)] = r
                zed[wave, c, :, col(ct)] = r * inverse[:, col(ct)]
        nears = [sideways(lambda ct, c=c: zed[wave, c, :, col(ct)], tiles) for c in range(2)]
        for ct in range(tiles):
            for c in range(2):
                near = next(nears[c])
                v = res[c, :, col(ct)] - (near + updown(zed[wave, c, :, col(ct)]))
                img[c, :, col(ct)] = v[:rows]
                yed[wave, c, :, col(ct)] = v * inverse[:, col(ct)]
        nears = [
            sideways(lambda ct, c=c: yed[wave, c, 0:rows, col(ct)], tiles) for c in range(2)
        ]
        sums = None
        for ct in range(tiles):
            r, v, w = [], [], []
            for c in range(2):
                near = next(nears[c])
                r.append(res[c, 0:rows, col(ct)])
                v.append(img[c, :, col(ct)])
                w.append(v[c] - (near + updown(yed[wave, c, :, col(ct)])[:rows]))
            found = [
                fold(r[0] * r[0] + r[1] * r[1]), *pair_products(r, v),
                fold(v[0] * v[0] + v[1] * v[1]), *pair_products(w, r), *pair_products(w, v),
                fold(w[0] * w[0] + w[1] * w[1]),
            ]
            sums = found if sums is None else [a + b for a, b in zip(sums, found)]
        for i, value in enumerate(sums):
            parts[i, pl.ds(wave, 1)] = jnp.sum(value, axis=0, keepdims=True)
        if with_overlap:
            away = mon_row[wave] - me * rows
            inside = jnp.where((away >= 0) & (away < rows), 1.0, 0.0)
            place = jnp.clip(away, 0, rows - 1)
            held = (
                lambda c: ext[field, wave, c, pl.ds(place, 1)],
                lambda c: zed[wave, c, pl.ds(place, 1)],
                lambda c: yed[wave, c, pl.ds(place, 1)],
            )
            for i, get in enumerate(held):
                sum_re = sum_im = None
                lines = [get(c) for c in range(2)]
                for ct in range(tiles):
                    m = [mon[wave, c : c + 1, col(ct)] for c in range(2)]
                    f = [line[:, col(ct)] for line in lines]
                    new_re = m[0] * f[0] + m[1] * f[1]
                    new_im = m[0] * f[1] - m[1] * f[0]
                    sum_re = new_re if sum_re is None else sum_re + new_re
                    sum_im = new_im if sum_im is None else sum_im + new_im
                parts[9 + 2 * i, pl.ds(wave, 1)] = inside * sum_re
                parts[10 + 2 * i, pl.ds(wave, 1)] = inside * sum_im

    def profile_row(profile, wave, turn, over):
        turn_c, turn_s = turn

        def row(ct):
            p = [profile[wave, c : c + 1, col(ct)] for c in range(2)]
            if over is not None:
                p_re, p_im = times(over, p)
                p = [p_re, -p_im]
            return turn_c * p[0] - turn_s * p[1], turn_s * p[0] + turn_c * p[1]

        return row

    def sum_over_gx(field):
        used = 15 if field == 0 else 9
        lane = lax.broadcasted_iota(jnp.int32, (waves, LANES), 1)
        packed = jnp.zeros((waves, LANES), jnp.float32)
        for i in range(used):
            packed = jnp.where(lane == i, jnp.sum(parts[i], axis=1, keepdims=True), packed)
        mine[field] = packed

        def move(hop, place):
            return pltpu.make_async_remote_copy(
                src_ref=mine.at[field], dst_ref=got.at[field, place],
                send_sem=sum_sems.at[0, field, hop], recv_sem=sum_sems.at[1, field, hop],
                device_id={"gx": lax.rem(me + hop, count)},
                device_id_type=pl.DeviceIdType.MESH,
            )

        for hop in range(1, count):
            move(hop, me).start()
        got[field, me] = packed
        for hop in range(1, count):
            move(hop, lax.rem(me - hop + count, count)).wait_recv()
        summed = got[field, 0]
        for place in range(1, count):
            summed = summed + got[field, place]
        for i, value in enumerate(scalars_of(summed, field == 0)):
            coef[field, i] = jnp.broadcast_to(value, (waves, LANES))
        for hop in range(1, count):
            move(hop, me).wait_send()

    def factors(field, wave, *slots):
        return [coef[field, i, pl.ds(wave, 1)] for i in slots]

    def result(field, wave, b, g, span):
        x = [ext[field, wave, c, 0:rows, span] for c in range(2)]
        z = [zed[wave, c, 0:rows, span] for c in range(2)]
        y = [yed[wave, c, 0:rows, span] for c in range(2)]
        bz, gy = times(b, z), times(g, y)
        return x[0] + bz[0] + gy[0], x[1] + bz[1] + gy[1]

    def forward_images(wave, carry):
        for way in range(2):
            halo_move(1, way, wave).start()
        for way in range(2):
            halo_move(0, way, wave).wait_recv()
        unpack(0, wave, 1.0)
        spot = spot_of(src_row[wave])
        images(0, wave, spot, profile_row(src, wave, turn_of(spot, wave, 1.0), None), True)
        return carry

    lax.fori_loop(0, waves, forward_images, 0)
    sum_over_gx(0)

    def adjoint_images(wave, carry):
        b, g, over = factors(0, wave, 0, 1), factors(0, wave, 2, 3), factors(0, wave, 4, 5)
        for ct in range(tiles):
            fwd[wave, 0, :, col(ct)], fwd[wave, 1, :, col(ct)] = result(0, wave, b, g, col(ct))
        for way in range(2):
            halo_move(1, way, wave).wait_recv()
        unpack(1, wave, -1.0)
        spot = spot_of(mon_row[wave])
        images(1, wave, spot, profile_row(mon, wave, turn_of(spot, wave, -1.0), over), False)
        return carry

    lax.fori_loop(0, waves, adjoint_images, 0)
    sum_over_gx(1)

    piece = width // depth

    def columns(place):
        return slice(place * piece, (place + 1) * piece)

    def scatter(hop, to, place):
        return pltpu.make_async_remote_copy(
            src_ref=gpart.at[to], dst_ref=ggot.at[place],
            send_sem=grad_sems.at[0, hop], recv_sem=grad_sems.at[1, hop],
            device_id={"wa": lax.rem(level + hop, depth)}, device_id_type=pl.DeviceIdType.MESH,
        )

    def gather(hop, place):
        return pltpu.make_async_remote_copy(
            src_ref=gtotal, dst_ref=gspread.at[place],
            send_sem=grad_sems.at[2, hop], recv_sem=grad_sems.at[3, hop],
            device_id={"wa": lax.rem(level + hop, depth)}, device_id_type=pl.DeviceIdType.MESH,
        )

    for place in range(depth):
        def finish(wave, terms):
            b, g = factors(1, wave, 0, 1), factors(1, wave, 2, 3)
            scale = 2.0 * wave_k[wave]
            fresh = []
            for i in range(piece // LANES):
                span = col(place * (piece // LANES) + i)
                out_re, out_im = result(1, wave, b, g, span)
                adj[wave, 0, :, span] = out_re
                adj[wave, 1, :, span] = out_im
                fresh.append(
                    terms[i] + scale * (out_re * fwd[wave, 0, :, span] - out_im * fwd[wave, 1, :, span])
                )
            return tuple(fresh)

        terms = lax.fori_loop(
            0, waves, finish,
            tuple(jnp.zeros((rows, LANES), jnp.float32) for _ in range(piece // LANES)),
        )
        for i, term in enumerate(terms):
            gpart[place, :, col(i)] = term
    for hop in range(1, depth):
        scatter(hop, lax.rem(level + hop, depth), level).start()
    ggot[level] = gpart[level]
    for hop in range(1, depth):
        from_place = lax.rem(level - hop + depth, depth)
        scatter(hop, from_place, from_place).wait_recv()
    summed = ggot[0]
    for place in range(1, depth):
        summed = summed + ggot[place]
    gtotal[...] = summed
    for hop in range(1, depth):
        gather(hop, level).start()
    gspread[level] = summed
    for hop in range(1, depth):
        gather(hop, lax.rem(level - hop + depth, depth)).wait_recv()
    for place in range(depth):
        grad[:, columns(place)] = mask[:, columns(place)].astype(jnp.float32) * gspread[place]
    for hop in range(1, depth):
        scatter(hop, lax.rem(level + hop, depth), level).wait_send()
        gather(hop, level).wait_send()
    for way in range(2):
        eps_move(way).wait_send()

    def drain(wave, carry):
        for field in range(2):
            for way in range(2):
                halo_move(field, way, wave).wait_send()
        return carry

    lax.fori_loop(0, waves, drain, 0)


def write_kernel(fwd_in, adj_in, grad_in, fwd, adj, grad, sems):
    waves = fwd_in.shape[0]
    copies = []
    for wave in range(waves):
        copies.append(pltpu.make_async_copy(fwd_in.at[wave], fwd.at[wave], sems.at[0, wave]))
        copies.append(pltpu.make_async_copy(adj_in.at[wave], adj.at[wave], sems.at[1, wave]))
    for copy in copies:
        copy.start()
    grad[...] = grad_in[...]
    for copy in copies:
        copy.wait()


def local(
    warm_field,
    warm_adjoint,
    permittivity,
    design_mask,
    source_row,
    monitor_row,
    wavenumber,
    bloch_phase,
    source_profile,
    monitor_profile,
):
    waves, _, rows, width = warm_field.shape
    total = rows + TILE
    count, depth = lax.axis_size("gx"), lax.axis_size("wa")
    turns = jnp.stack([jnp.cos(bloch_phase), jnp.sin(bloch_phase)])

    smem = pl.BlockSpec(memory_space=pltpu.SMEM)
    vmem = pl.BlockSpec(memory_space=pltpu.VMEM)
    anywhere = pl.BlockSpec(memory_space=pl.ANY)
    f32 = jnp.float32
    piece = (rows, width // depth)
    block = (2 * REACH * QUARTERS, width // QUARTERS)
    fwd, adj, grad = pl.pallas_call(
        functools.partial(step_kernel, count, depth),
        out_shape=(
            pltpu.VMEM(warm_field.shape, f32),
            pltpu.VMEM(warm_field.shape, f32),
            pltpu.VMEM((rows, width), f32),
        ),
        in_specs=[smem] * 4 + [anywhere] * 6,
        out_specs=(vmem, vmem, vmem),
        scratch_shapes=[
            pltpu.VMEM((2, waves, 2, total, width), f32),
            pltpu.VMEM((waves, 2, total, width), f32),
            pltpu.VMEM((waves, 2, total, width), f32),
            pltpu.VMEM((2, 2, waves, *block), f32),
            pltpu.VMEM((2, 2, waves, *block), f32),
            pltpu.VMEM((2, total, width), f32),
            pltpu.VMEM((2, rows, width), f32),
            pltpu.VMEM((total, width), f32),
            pltpu.VMEM((total, width), f32),
            pltpu.VMEM((total, width), f32),
            pltpu.VMEM((2, 4 * QUARTERS, width // QUARTERS), f32),
            pltpu.VMEM((2, 4 * QUARTERS, width // QUARTERS), f32),
            pltpu.VMEM(source_profile.shape, f32),
            pltpu.VMEM(monitor_profile.shape, f32),
            pltpu.VMEM((rows, width), jnp.int32),
            pltpu.VMEM((SUMS, waves, LANES), f32),
            pltpu.VMEM((2, waves, LANES), f32),
            pltpu.VMEM((2, count, waves, LANES), f32),
            pltpu.VMEM((2, 6, waves, LANES), f32),
            pltpu.VMEM((depth, *piece), f32),
            pltpu.VMEM((depth, *piece), f32),
            pltpu.VMEM(piece, f32),
            pltpu.VMEM((depth, *piece), f32),
            pltpu.SemaphoreType.DMA((2, waves)),
            pltpu.SemaphoreType.DMA((4,)),
            pltpu.SemaphoreType.DMA((2, 2, 2, waves)),
            pltpu.SemaphoreType.DMA((2, 2)),
            pltpu.SemaphoreType.DMA((2, 2, count)),
            pltpu.SemaphoreType.DMA((4, depth)),
        ],
        compiler_params=pltpu.CompilerParams(
            collective_id=0, has_side_effects=True, vmem_limit_bytes=VMEM_LIMIT
        ),
        name="step",
    )(
        turns, wavenumber, source_row, monitor_row, permittivity, warm_field, warm_adjoint,
        design_mask, source_profile, monitor_profile,
    )
    field_shape = jax.ShapeDtypeStruct(warm_field.shape, f32)
    return pl.pallas_call(
        write_kernel,
        out_shape=(field_shape, field_shape, jax.ShapeDtypeStruct((rows, width), f32)),
        in_specs=[vmem, vmem, vmem],
        out_specs=(anywhere, anywhere, vmem),
        scratch_shapes=[pltpu.SemaphoreType.DMA((2, waves))],
        compiler_params=pltpu.CompilerParams(vmem_limit_bytes=1024 * 1024),
        name="write_out",
    )(fwd, adj, grad)


def solution(mesh):
    placed = (
        P("wa", None, "gx", None),
        P("wa", None, "gx", None),
        P("gx", None),
        P("gx", None),
        P("wa"),
        P("wa"),
        P("wa"),
        P("wa"),
        P("wa", None, None),
        P("wa", None, None),
    )
    return jax.shard_map(
        local,
        mesh=mesh,
        in_specs=placed,
        out_specs=(P("wa", None, "gx", None), P("wa", None, "gx", None), P("gx", None)),
        check_vma=False,
    )
```

```python
import functools

import jax
import jax.numpy as jnp
from jax import lax
from jax.experimental import pallas as pl
from jax.experimental.pallas import tpu as pltpu
from jax.sharding import PartitionSpec as P

floor_share = 0.5
REACH = 3
TILE = 8
LANES = 128
QUARTERS = 4
SUMS = 16
GROUPS = 2
VMEM_LIMIT = 50000 * 1024


def col(tile):
    return slice(tile * LANES, (tile + 1) * LANES)


def sideways(load, tiles):
    tile = load(0)
    lane = lax.broadcasted_iota(jnp.int32, tile.shape, 1)
    at_right, at_left = lane == LANES - 1, lane == 0
    after, before = pltpu.roll(tile, LANES - 1, 1), pltpu.roll(tile, 1, 1)
    carried = jnp.zeros_like(tile)
    for ct in range(tiles):
        if ct + 1 < tiles:
            ahead = load(ct + 1)
            next_after, next_before = pltpu.roll(ahead, LANES - 1, 1), pltpu.roll(ahead, 1, 1)
        else:
            ahead, next_after, next_before = None, jnp.zeros_like(tile), None
        near = jnp.where(at_right, next_after, after) + jnp.where(at_left, carried, before)
        yield near
        carried, tile, after, before = before, ahead, next_after, next_before


def updown(tile):
    total = tile.shape[0]
    return pltpu.roll(tile, total - 1, 0) + pltpu.roll(tile, 1, 0)


def fold(cells):
    acc = cells[:TILE]
    for start in range(TILE, cells.shape[0], TILE):
        acc = acc + cells[start : start + TILE]
    return acc


def pair_products(a, b):
    return fold(a[0] * b[0] + a[1] * b[1]), fold(a[0] * b[1] - a[1] * b[0])


def times(a, b):
    return a[0] * b[0] - a[1] * b[1], a[0] * b[1] + a[1] * b[0]


def scalars_of(total, with_overlap):
    q = [total[:, i : i + 1] for i in range(SUMS)]
    res_norm, rv_re, rv_im, image_sq, wr_re, wr_im, wv_re, wv_im, twice_sq = q[:9]
    half = floor_share * res_norm
    bounded = jnp.maximum(rv_re * rv_re + rv_im * rv_im, half * half)
    step_re = res_norm * rv_re / bounded
    step_im = -res_norm * rv_im / bounded
    step_sq = step_re * step_re + step_im * step_im
    ts_re = rv_re - step_re * image_sq - (step_re * wr_re + step_im * wr_im) + step_sq * wv_re
    ts_im = -rv_im - step_im * image_sq - (step_re * wr_im - step_im * wr_re) + step_sq * wv_im
    tt_sum = image_sq - 2.0 * (step_re * wv_re + step_im * wv_im) + step_sq * twice_sq
    omega_re = ts_re / tt_sum
    omega_im = ts_im / tt_sum
    both_re, both_im = times((step_re, step_im), (omega_re, omega_im))
    found = [step_re + omega_re, step_im + omega_im, -both_re, -both_im]
    if with_overlap:
        mx_re, mx_im, mz_re, mz_im, my_re, my_im = q[9:15]
        for_z = times(found[0:2], (mz_re, mz_im))
        for_y = times(found[2:4], (my_re, my_im))
        found.append(mx_re + for_z[0] + for_y[0])
        found.append(mx_im + for_z[1] + for_y[1])
    return found


def step_kernel(
    count, depth,
    phase_hbm, wave_hbm, src_row_hbm, mon_row_hbm, eps_hbm, field_hbm, adjoint_hbm, mask_hbm, src_hbm, mon_hbm,
    fwd, adj, grad,
    ext, zed, yed, send, recv, res, img, diag, inverse, eps, eps_send, eps_recv, src, mon, mask,
    phase, wave_k, src_row, mon_row, turns, parts, mine, got, coef, gpart, ggot, gtotal, gspread,
    load_sem, side_sem, halo_sems, eps_sems, sum_sems, grad_sems,
):
    waves, _, rows, width = field_hbm.shape
    total = rows + TILE
    tiles = width // LANES
    quarter = width // QUARTERS
    half = waves // GROUPS
    whole = rows * count
    me = lax.axis_index("gx")
    level = lax.axis_index("wa")
    before, after = lax.rem(me - 1 + count, count), lax.rem(me + 1, count)
    at_first, at_last = me == 0, me == count - 1

    fields = (field_hbm, adjoint_hbm)

    def load(field, wave):
        return pltpu.make_async_copy(
            fields[field].at[wave], ext.at[field, wave, :, pl.ds(0, rows)],
            load_sem.at[field, wave],
        )

    sides = [
        pltpu.make_async_copy(eps_hbm, eps.at[pl.ds(0, rows)], side_sem.at[0]),
        pltpu.make_async_copy(src_hbm, src, side_sem.at[1]),
        pltpu.make_async_copy(mon_hbm, mon, side_sem.at[2]),
        pltpu.make_async_copy(mask_hbm, mask, side_sem.at[3]),
    ]
    scalars = [
        pltpu.make_async_copy(phase_hbm, phase, side_sem.at[4]),
        pltpu.make_async_copy(wave_hbm, wave_k, side_sem.at[5]),
        pltpu.make_async_copy(src_row_hbm, src_row, side_sem.at[6]),
        pltpu.make_async_copy(mon_row_hbm, mon_row, side_sem.at[7]),
    ]
    barrier = pltpu.get_barrier_semaphore()
    for axis, size, own in (("wa", depth, level), ("gx", count, me)):
        for hop in range(1, size):
            pl.semaphore_signal(
                barrier, inc=1, device_id={axis: lax.rem(own + hop, size)},
                device_id_type=pl.DeviceIdType.MESH,
            )
    sides[0].start()
    for wave in range(waves):
        load(0, wave).start()
    for copy in scalars + sides[1:]:
        copy.start()

    sides[0].wait()
    for way, low in ((0, 0), (1, rows - 2)):
        for part in range(QUARTERS):
            span = slice(part * quarter, (part + 1) * quarter)
            eps_send[way, part * 2 : part * 2 + 2] = eps[low : low + 2, span]

    def neighbour(way):
        return {"gx": before if way == 0 else after}

    def eps_move(way):
        return pltpu.make_async_remote_copy(
            src_ref=eps_send.at[way], dst_ref=eps_recv.at[way],
            send_sem=eps_sems.at[0, way], recv_sem=eps_sems.at[1, way],
            device_id=neighbour(way), device_id_type=pl.DeviceIdType.MESH,
        )

    def halo_move(field, way, wave):
        return pltpu.make_async_remote_copy(
            src_ref=send.at[field, way, wave], dst_ref=recv.at[field, way, wave],
            send_sem=halo_sems.at[0, field, way, wave],
            recv_sem=halo_sems.at[1, field, way, wave],
            device_id=neighbour(way), device_id_type=pl.DeviceIdType.MESH,
        )

    def pack(field, wave):
        for way, low in ((0, 0), (1, rows - REACH)):
            for c in range(2):
                for part in range(QUARTERS):
                    span = slice(part * quarter, (part + 1) * quarter)
                    at = part * 2 * REACH + c * REACH
                    send[field, way, wave, at : at + REACH] = ext[
                        field, wave, c, low : low + REACH, span
                    ]

    pl.semaphore_wait(barrier, count - 1 + depth - 1)
    for way in range(2):
        eps_move(way).start()

    def first_sends(wave, carry):
        load(0, wave).wait()
        pack(0, wave)
        for way in range(2):
            halo_move(0, way, wave).start()
        return carry

    lax.fori_loop(0, waves, first_sends, 0)
    for wave in range(waves):
        load(1, wave).start()
    for copy in scalars + sides[1:]:
        copy.wait()
    wave_of = lax.broadcasted_iota(jnp.int32, (waves, LANES), 0)
    angle = jnp.zeros((waves, LANES), jnp.float32)
    for wave in range(waves):
        angle = jnp.where(wave_of == wave, phase[wave], angle)
    turns[0], turns[1] = jnp.cos(angle), jnp.sin(angle)

    def adjoint_packs(wave, carry):
        load(1, wave).wait()
        pack(1, wave)
        return carry

    lax.fori_loop(0, waves, adjoint_packs, 0)

    eps[rows:] = jnp.ones((TILE, width), jnp.float32)
    for way, at in ((0, rows), (1, total - 2)):
        eps_move(way).wait_recv()
        for part in range(QUARTERS):
            span = slice(part * quarter, (part + 1) * quarter)
            eps[at : at + 2, span] = eps_recv[way, part * 2 : part * 2 + 2]

    row_of = lax.broadcasted_iota(jnp.int32, (total, LANES), 0)

    def spot_of(row):
        away = row - me * rows
        away = jnp.where(away < 0, away + whole, away)
        spot = jnp.where(
            away < rows + REACH, away,
            jnp.where(away >= whole - REACH, away - whole + total, -1),
        )
        return spot

    def turn_of(spot, wave, sign):
        cosine, sine = turns[0, pl.ds(wave, 1)], sign * turns[1, pl.ds(wave, 1)]
        above = (spot >= rows) & (spot < rows + REACH) & at_last
        below = (spot >= rows + REACH) & at_first
        turn_c = jnp.where(above | below, cosine, 1.0)
        turn_s = jnp.where(above, sine, jnp.where(below, -sine, 0.0))
        return turn_c, turn_s

    def unpack(field, wave, sign):
        cosine, sine = turns[0, pl.ds(wave, 1)], sign * turns[1, pl.ds(wave, 1)]
        for way, at in ((0, rows), (1, total - REACH)):
            edge = at_last if way == 0 else at_first
            turn_c = jnp.where(edge, cosine, 1.0)
            turn_s = jnp.where(edge, sine if way == 0 else -sine, 0.0)
            for ct in range(tiles):
                base, place = 2 * REACH * (ct // (tiles // QUARTERS)), col(ct % (tiles // QUARTERS))
                got_re = recv[field, way, wave, base : base + REACH, place]
                got_im = recv[field, way, wave, base + REACH : base + 2 * REACH, place]
                ext[field, wave, 0, at : at + REACH, col(ct)] = turn_c * got_re - turn_s * got_im
                ext[field, wave, 1, at : at + REACH, col(ct)] = turn_s * got_re + turn_c * got_im

    def images(field, wave, spot, side_row, with_overlap):
        squared_k = wave_k[wave]
        for ct in range(tiles):
            d = 4.0 - squared_k * eps[:, col(ct)]
            diag[:, col(ct)] = d
            inverse[:, col(ct)] = 1.0 / d
        here = row_of == spot
        nears = [
            sideways(lambda ct, c=c: ext[field, wave, c, :, col(ct)], tiles) for c in range(2)
        ]
        for ct in range(tiles):
            rows_in = side_row(ct)
            for c in range(2):
                near = next(nears[c])
                x = ext[field, wave, c, :, col(ct)]
                r = (near + updown(x)) - diag[:, col(ct)] * x
                r = jnp.where(here, r + rows_in[c], r)
                res[c, :, col(ct)] = r
                zed[wave, c, :, col(ct)] = r * inverse[:, col(ct)]
        nears = [sideways(lambda ct, c=c: zed[wave, c, :, col(ct)], tiles) for c in range(2)]
        for ct in range(tiles):
            for c in range(2):
                near = next(nears[c])
                v = res[c, :, col(ct)] - (near + updown(zed[wave, c, :, col(ct)]))
                img[c, :, col(ct)] = v[:rows]
                yed[wave, c, :, col(ct)] = v * inverse[:, col(ct)]
        nears = [
            sideways(lambda ct, c=c: yed[wave, c, 0:rows, col(ct)], tiles) for c in range(2)
        ]
        sums = None
        for ct in range(tiles):
            r, v, w = [], [], []
            for c in range(2):
                near = next(nears[c])
                r.append(res[c, 0:rows, col(ct)])
                v.append(img[c, :, col(ct)])
                w.append(v[c] - (near + updown(yed[wave, c, :, col(ct)])[:rows]))
            found = [
                fold(r[0] * r[0] + r[1] * r[1]), *pair_products(r, v),
                fold(v[0] * v[0] + v[1] * v[1]), *pair_products(w, r), *pair_products(w, v),
                fold(w[0] * w[0] + w[1] * w[1]),
            ]
            sums = found if sums is None else [a + b for a, b in zip(sums, found)]
        for i, value in enumerate(sums):
            parts[i, pl.ds(wave, 1)] = jnp.sum(value, axis=0, keepdims=True)
        if with_overlap:
            away = mon_row[wave] - me * rows
            inside = jnp.where((away >= 0) & (away < rows), 1.0, 0.0)
            place = jnp.clip(away, 0, rows - 1)
            held = (
                lambda c: ext[field, wave, c, pl.ds(place, 1)],
                lambda c: zed[wave, c, pl.ds(place, 1)],
                lambda c: yed[wave, c, pl.ds(place, 1)],
            )
            for i, get in enumerate(held):
                sum_re = sum_im = None
                lines = [get(c) for c in range(2)]
                for ct in range(tiles):
                    m = [mon[wave, c : c + 1, col(ct)] for c in range(2)]
                    f = [line[:, col(ct)] for line in lines]
                    new_re = m[0] * f[0] + m[1] * f[1]
                    new_im = m[0] * f[1] - m[1] * f[0]
                    sum_re = new_re if sum_re is None else sum_re + new_re
                    sum_im = new_im if sum_im is None else sum_im + new_im
                parts[9 + 2 * i, pl.ds(wave, 1)] = inside * sum_re
                parts[10 + 2 * i, pl.ds(wave, 1)] = inside * sum_im

    def profile_row(profile, wave, turn, over):
        turn_c, turn_s = turn

        def row(ct):
            p = [profile[wave, c : c + 1, col(ct)] for c in range(2)]
            if over is not None:
                p_re, p_im = times(over, p)
                p = [p_re, -p_im]
            return turn_c * p[0] - turn_s * p[1], turn_s * p[0] + turn_c * p[1]

        return row

    def sum_move(field, group, hop, place):
        return pltpu.make_async_remote_copy(
            src_ref=mine.at[field, group], dst_ref=got.at[field, group, place],
            send_sem=sum_sems.at[0, field, group, hop], recv_sem=sum_sems.at[1, field, group, hop],
            device_id={"gx": lax.rem(me + hop, count)}, device_id_type=pl.DeviceIdType.MESH,
        )

    def send_sums(field, group):
        used = 15 if field == 0 else 9
        lane = lax.broadcasted_iota(jnp.int32, (half, LANES), 1)
        packed = jnp.zeros((half, LANES), jnp.float32)
        members = pl.ds(pl.multiple_of(group * half, half), half)
        for i in range(used):
            packed = jnp.where(lane == i, jnp.sum(parts[i, members], axis=1, keepdims=True), packed)
        mine[field, group] = packed
        got[field, group, me] = packed
        for hop in range(1, count):
            sum_move(field, group, hop, me).start()

    def take_sums(field, group):
        for hop in range(1, count):
            sum_move(field, group, hop, lax.rem(me - hop + count, count)).wait_recv()
        summed = got[field, group, 0]
        for place in range(1, count):
            summed = summed + got[field, group, place]
        members = pl.ds(pl.multiple_of(group * half, half), half)
        for i, value in enumerate(scalars_of(summed, field == 0)):
            coef[field, i, members] = jnp.broadcast_to(value, (half, LANES))

    def factors(field, wave, *slots):
        return [coef[field, i, pl.ds(wave, 1)] for i in slots]

    def result(field, wave, b, g, span):
        x = [ext[field, wave, c, 0:rows, span] for c in range(2)]
        z = [zed[wave, c, 0:rows, span] for c in range(2)]
        y = [yed[wave, c, 0:rows, span] for c in range(2)]
        bz, gy = times(b, z), times(g, y)
        return x[0] + bz[0] + gy[0], x[1] + bz[1] + gy[1]

    def forward_images(wave, carry):
        for way in range(2):
            halo_move(0, way, wave).wait_recv()
        unpack(0, wave, 1.0)
        spot = spot_of(src_row[wave])
        images(0, wave, spot, profile_row(src, wave, turn_of(spot, wave, 1.0), None), True)
        return carry

    def adjoint_sends(wave, carry):
        for way in range(2):
            halo_move(1, way, wave).start()
        return carry

    def forward_group(group, carry):
        lax.fori_loop(group * half, (group + 1) * half, forward_images, 0)
        send_sums(0, group)
        lax.fori_loop(group * half, (group + 1) * half, adjoint_sends, 0)
        return carry

    lax.fori_loop(0, GROUPS, forward_group, 0)

    def adjoint_images(wave, carry):
        b, g, over = factors(0, wave, 0, 1), factors(0, wave, 2, 3), factors(0, wave, 4, 5)
        for ct in range(tiles):
            fwd[wave, 0, :, col(ct)], fwd[wave, 1, :, col(ct)] = result(0, wave, b, g, col(ct))
        for way in range(2):
            halo_move(1, way, wave).wait_recv()
        unpack(1, wave, -1.0)
        spot = spot_of(mon_row[wave])
        images(1, wave, spot, profile_row(mon, wave, turn_of(spot, wave, -1.0), over), False)
        return carry

    def adjoint_group(group, carry):
        take_sums(0, group)
        lax.fori_loop(group * half, (group + 1) * half, adjoint_images, 0)
        send_sums(1, group)
        return carry

    lax.fori_loop(0, GROUPS, adjoint_group, 0)

    piece = width // depth

    def columns(place):
        return slice(place * piece, (place + 1) * piece)

    def scatter(hop, place):
        return pltpu.make_async_remote_copy(
            src_ref=gpart.at[hop], dst_ref=ggot.at[place],
            send_sem=grad_sems.at[0, hop], recv_sem=grad_sems.at[1, hop],
            device_id={"wa": lax.rem(level + hop, depth)}, device_id_type=pl.DeviceIdType.MESH,
        )

    def gather(hop, place):
        return pltpu.make_async_remote_copy(
            src_ref=gtotal, dst_ref=gspread.at[place],
            send_sem=grad_sems.at[2, hop], recv_sem=grad_sems.at[3, hop],
            device_id={"wa": lax.rem(level + hop, depth)}, device_id_type=pl.DeviceIdType.MESH,
        )

    hops = [*range(1, depth), 0]
    for group in range(GROUPS):
        take_sums(1, group)
        for hop in hops:
            base = lax.rem(level + hop, depth) * piece
            spans = [
                pl.ds(pl.multiple_of(base + i * LANES, LANES), LANES)
                for i in range(piece // LANES)
            ]

            def finish(wave, terms):
                b, g = factors(1, wave, 0, 1), factors(1, wave, 2, 3)
                scale = 2.0 * wave_k[wave]
                fresh = []
                for span, term in zip(spans, terms):
                    out_re, out_im = result(1, wave, b, g, span)
                    adj[wave, 0, :, span] = out_re
                    adj[wave, 1, :, span] = out_im
                    fwd_re, fwd_im = fwd[wave, 0, :, span], fwd[wave, 1, :, span]
                    fresh.append(term + scale * (out_re * fwd_re - out_im * fwd_im))
                return tuple(fresh)

            zero = jnp.zeros((rows, LANES), jnp.float32)
            terms = lax.fori_loop(
                group * half, (group + 1) * half, finish,
                tuple(gpart[hop, :, col(i)] if group else zero for i in range(piece // LANES)),
            )
            for i, term in enumerate(terms):
                gpart[hop, :, col(i)] = term
            if group == GROUPS - 1 and hop:
                scatter(hop, level).start()
    ggot[level] = gpart[0]
    for hop in range(1, depth):
        scatter(hop, lax.rem(level - hop + depth, depth)).wait_recv()
    summed = ggot[0]
    for place in range(1, depth):
        summed = summed + ggot[place]
    gtotal[...] = summed
    for hop in range(1, depth):
        gather(hop, level).start()
    gspread[level] = summed
    for hop in range(1, depth):
        gather(hop, lax.rem(level - hop + depth, depth)).wait_recv()
    for place in range(depth):
        grad[:, columns(place)] = mask[:, columns(place)].astype(jnp.float32) * gspread[place]
    for hop in range(1, depth):
        scatter(hop, level).wait_send()
        gather(hop, level).wait_send()
    for way in range(2):
        eps_move(way).wait_send()

    def drain(wave, carry):
        for field in range(2):
            for way in range(2):
                halo_move(field, way, wave).wait_send()
        return carry

    lax.fori_loop(0, waves, drain, 0)
    for field in range(2):
        for group in range(GROUPS):
            for hop in range(1, count):
                sum_move(field, group, hop, me).wait_send()


def write_kernel(fwd_in, adj_in, grad_in, fwd, adj, grad, sems):
    waves = fwd_in.shape[0]
    copies = []
    for wave in range(waves):
        copies.append(pltpu.make_async_copy(fwd_in.at[wave], fwd.at[wave], sems.at[0, wave]))
        copies.append(pltpu.make_async_copy(adj_in.at[wave], adj.at[wave], sems.at[1, wave]))
    copies.append(pltpu.make_async_copy(grad_in, grad, sems.at[0, waves]))
    for copy in copies:
        copy.start()
    for copy in copies:
        copy.wait()


def local(
    warm_field,
    warm_adjoint,
    permittivity,
    design_mask,
    source_row,
    monitor_row,
    wavenumber,
    bloch_phase,
    source_profile,
    monitor_profile,
):
    waves, _, rows, width = warm_field.shape
    total = rows + TILE
    count, depth = lax.axis_size("gx"), lax.axis_size("wa")

    vmem = pl.BlockSpec(memory_space=pltpu.VMEM)
    anywhere = pl.BlockSpec(memory_space=pl.ANY)
    f32 = jnp.float32
    piece = (rows, width // depth)
    block = (2 * REACH * QUARTERS, width // QUARTERS)
    fwd, adj, grad = pl.pallas_call(
        functools.partial(step_kernel, count, depth),
        out_shape=(
            pltpu.VMEM(warm_field.shape, f32),
            pltpu.VMEM(warm_field.shape, f32),
            pltpu.VMEM((rows, width), f32),
        ),
        in_specs=[anywhere] * 10,
        out_specs=(vmem, vmem, vmem),
        scratch_shapes=[
            pltpu.VMEM((2, waves, 2, total, width), f32),
            pltpu.VMEM((waves, 2, total, width), f32),
            pltpu.VMEM((waves, 2, total, width), f32),
            pltpu.VMEM((2, 2, waves, *block), f32),
            pltpu.VMEM((2, 2, waves, *block), f32),
            pltpu.VMEM((2, total, width), f32),
            pltpu.VMEM((2, rows, width), f32),
            pltpu.VMEM((total, width), f32),
            pltpu.VMEM((total, width), f32),
            pltpu.VMEM((total, width), f32),
            pltpu.VMEM((2, 2 * QUARTERS, width // QUARTERS), f32),
            pltpu.VMEM((2, 2 * QUARTERS, width // QUARTERS), f32),
            pltpu.VMEM(source_profile.shape, f32),
            pltpu.VMEM(monitor_profile.shape, f32),
            pltpu.VMEM((rows, width), jnp.int32),
            pltpu.SMEM((waves,), f32),
            pltpu.SMEM((waves,), f32),
            pltpu.SMEM((waves,), jnp.int32),
            pltpu.SMEM((waves,), jnp.int32),
            pltpu.VMEM((2, waves, LANES), f32),
            pltpu.VMEM((SUMS, waves, LANES), f32),
            pltpu.VMEM((2, GROUPS, waves // GROUPS, LANES), f32),
            pltpu.VMEM((2, GROUPS, count, waves // GROUPS, LANES), f32),
            pltpu.VMEM((2, 6, waves, LANES), f32),
            pltpu.VMEM((depth, *piece), f32),
            pltpu.VMEM((depth, *piece), f32),
            pltpu.VMEM(piece, f32),
            pltpu.VMEM((depth, *piece), f32),
            pltpu.SemaphoreType.DMA((2, waves)),
            pltpu.SemaphoreType.DMA((8,)),
            pltpu.SemaphoreType.DMA((2, 2, 2, waves)),
            pltpu.SemaphoreType.DMA((2, 2)),
            pltpu.SemaphoreType.DMA((2, 2, GROUPS, count)),
            pltpu.SemaphoreType.DMA((4, depth)),
        ],
        compiler_params=pltpu.CompilerParams(
            collective_id=0, has_side_effects=True, vmem_limit_bytes=VMEM_LIMIT
        ),
        name="step",
    )(
        bloch_phase, wavenumber, source_row, monitor_row, permittivity, warm_field, warm_adjoint,
        design_mask, source_profile, monitor_profile,
    )
    field_shape = jax.ShapeDtypeStruct(warm_field.shape, f32)
    return pl.pallas_call(
        write_kernel,
        out_shape=(field_shape, field_shape, jax.ShapeDtypeStruct((rows, width), f32)),
        in_specs=[vmem, vmem, vmem],
        out_specs=(anywhere, anywhere, anywhere),
        scratch_shapes=[pltpu.SemaphoreType.DMA((2, waves + 1))],
        compiler_params=pltpu.CompilerParams(vmem_limit_bytes=1024 * 1024),
        name="write_out",
    )(fwd, adj, grad)


def solution(mesh):
    placed = (
        P("wa", None, "gx", None),
        P("wa", None, "gx", None),
        P("gx", None),
        P("gx", None),
        P("wa"),
        P("wa"),
        P("wa"),
        P("wa"),
        P("wa", None, None),
        P("wa", None, None),
    )
    return jax.shard_map(
        local,
        mesh=mesh,
        in_specs=placed,
        out_specs=(P("wa", None, "gx", None), P("wa", None, "gx", None), P("gx", None)),
        check_vma=False,
    )
```

```python
import functools

import jax
import jax.numpy as jnp
from jax import lax
from jax.experimental import pallas as pl
from jax.experimental.pallas import tpu as pltpu
from jax.sharding import PartitionSpec as P

floor_share = 0.5
REACH = 3
TILE = 8
LANES = 128
QUARTERS = 4
SUMS = 16
GROUPS = 4
VMEM_LIMIT = 50000 * 1024


def col(tile):
    return slice(tile * LANES, (tile + 1) * LANES)


def sideways(load, tiles):
    tile = load(0)
    lane = lax.broadcasted_iota(jnp.int32, tile.shape, 1)
    at_right, at_left = lane == LANES - 1, lane == 0
    after, before = pltpu.roll(tile, LANES - 1, 1), pltpu.roll(tile, 1, 1)
    carried = jnp.zeros_like(tile)
    for ct in range(tiles):
        if ct + 1 < tiles:
            ahead = load(ct + 1)
            next_after, next_before = pltpu.roll(ahead, LANES - 1, 1), pltpu.roll(ahead, 1, 1)
        else:
            ahead, next_after, next_before = None, jnp.zeros_like(tile), None
        near = jnp.where(at_right, next_after, after) + jnp.where(at_left, carried, before)
        yield near
        carried, tile, after, before = before, ahead, next_after, next_before


def updown(tile):
    total = tile.shape[0]
    return pltpu.roll(tile, total - 1, 0) + pltpu.roll(tile, 1, 0)


def fold(cells):
    acc = cells[:TILE]
    for start in range(TILE, cells.shape[0], TILE):
        acc = acc + cells[start : start + TILE]
    return acc


def pair_products(a, b):
    return fold(a[0] * b[0] + a[1] * b[1]), fold(a[0] * b[1] - a[1] * b[0])


def times(a, b):
    return a[0] * b[0] - a[1] * b[1], a[0] * b[1] + a[1] * b[0]


def scalars_of(total, with_overlap):
    q = [total[:, i : i + 1] for i in range(SUMS)]
    res_norm, rv_re, rv_im, image_sq, wr_re, wr_im, wv_re, wv_im, twice_sq = q[:9]
    half = floor_share * res_norm
    bounded = jnp.maximum(rv_re * rv_re + rv_im * rv_im, half * half)
    step_re = res_norm * rv_re / bounded
    step_im = -res_norm * rv_im / bounded
    step_sq = step_re * step_re + step_im * step_im
    ts_re = rv_re - step_re * image_sq - (step_re * wr_re + step_im * wr_im) + step_sq * wv_re
    ts_im = -rv_im - step_im * image_sq - (step_re * wr_im - step_im * wr_re) + step_sq * wv_im
    tt_sum = image_sq - 2.0 * (step_re * wv_re + step_im * wv_im) + step_sq * twice_sq
    omega_re = ts_re / tt_sum
    omega_im = ts_im / tt_sum
    both_re, both_im = times((step_re, step_im), (omega_re, omega_im))
    found = [step_re + omega_re, step_im + omega_im, -both_re, -both_im]
    if with_overlap:
        mx_re, mx_im, mz_re, mz_im, my_re, my_im = q[9:15]
        for_z = times(found[0:2], (mz_re, mz_im))
        for_y = times(found[2:4], (my_re, my_im))
        found.append(mx_re + for_z[0] + for_y[0])
        found.append(mx_im + for_z[1] + for_y[1])
    return found


def step_kernel(
    count, depth,
    phase_hbm, wave_hbm, src_row_hbm, mon_row_hbm, eps_hbm, field_hbm, adjoint_hbm, mask_hbm, src_hbm, mon_hbm,
    fwd, adj, grad,
    ext, zed, yed, send, recv, res, img, diag, inverse, eps, eps_send, eps_recv, src, mon, mask,
    phase, wave_k, src_row, mon_row, turns, parts, mine, got, coef, gpart, ggot, gtotal, gspread,
    load_sem, side_sem, sent_sem, halo_sem, eps_sems, sum_sems, grad_sems,
):
    waves, _, rows, width = field_hbm.shape
    total = rows + TILE
    tiles = width // LANES
    quarter = width // QUARTERS
    size = waves // GROUPS
    whole = rows * count
    me = lax.axis_index("gx")
    level = lax.axis_index("wa")
    before, after = lax.rem(me - 1 + count, count), lax.rem(me + 1, count)
    at_first, at_last = me == 0, me == count - 1

    fields = (field_hbm, adjoint_hbm)

    def load(field, group):
        members = pl.ds(group * size, size)
        return pltpu.make_async_copy(
            fields[field].at[members], ext.at[field, members, :, pl.ds(0, rows)],
            load_sem.at[field, group],
        )

    sides = [
        pltpu.make_async_copy(eps_hbm, eps.at[pl.ds(0, rows)], side_sem.at[0]),
        pltpu.make_async_copy(src_hbm, src, side_sem.at[1]),
        pltpu.make_async_copy(mon_hbm, mon, side_sem.at[2]),
        pltpu.make_async_copy(mask_hbm, mask, side_sem.at[3]),
    ]
    scalars = [
        pltpu.make_async_copy(phase_hbm, phase, side_sem.at[4]),
        pltpu.make_async_copy(wave_hbm, wave_k, side_sem.at[5]),
        pltpu.make_async_copy(src_row_hbm, src_row, side_sem.at[6]),
        pltpu.make_async_copy(mon_row_hbm, mon_row, side_sem.at[7]),
    ]
    barrier = pltpu.get_barrier_semaphore()
    for axis, extent, own in (("wa", depth, level), ("gx", count, me)):
        for hop in range(1, extent):
            pl.semaphore_signal(
                barrier, inc=1, device_id={axis: lax.rem(own + hop, extent)},
                device_id_type=pl.DeviceIdType.MESH,
            )
    sides[0].start()
    for group in range(GROUPS):
        load(0, group).start()
    for copy in scalars + sides[1:]:
        copy.start()

    sides[0].wait()
    for way, low in ((0, 0), (1, rows - 2)):
        for part in range(QUARTERS):
            span = slice(part * quarter, (part + 1) * quarter)
            eps_send[way, part * 2 : part * 2 + 2] = eps[low : low + 2, span]

    def neighbour(way):
        return {"gx": before if way == 0 else after}

    def eps_move(way):
        return pltpu.make_async_remote_copy(
            src_ref=eps_send.at[way], dst_ref=eps_recv.at[way],
            send_sem=eps_sems.at[0, way], recv_sem=eps_sems.at[1, way],
            device_id=neighbour(way), device_id_type=pl.DeviceIdType.MESH,
        )

    def halo_move(field, way, wave):
        return pltpu.make_async_remote_copy(
            src_ref=send.at[field, way, wave], dst_ref=recv.at[field, way, wave],
            send_sem=sent_sem.at[field, way], recv_sem=halo_sem.at[field, way, wave],
            device_id=neighbour(way), device_id_type=pl.DeviceIdType.MESH,
        )

    def halos_sent(field, way):
        return pltpu.make_async_remote_copy(
            src_ref=send.at[field, way], dst_ref=recv.at[field, way],
            send_sem=sent_sem.at[field, way], recv_sem=halo_sem.at[field, way, 0],
            device_id=neighbour(way), device_id_type=pl.DeviceIdType.MESH,
        )

    def pack(field, wave):
        for way, low in ((0, 0), (1, rows - REACH)):
            for c in range(2):
                for part in range(QUARTERS):
                    span = slice(part * quarter, (part + 1) * quarter)
                    at = part * 2 * REACH + c * REACH
                    send[field, way, wave, at : at + REACH] = ext[
                        field, wave, c, low : low + REACH, span
                    ]

    pl.semaphore_wait(barrier, count - 1 + depth - 1)
    for way in range(2):
        eps_move(way).start()

    def first_sends(group, carry):
        load(0, group).wait()

        def each(wave, carry):
            pack(0, wave)
            for way in range(2):
                halo_move(0, way, wave).start()
            return carry

        return lax.fori_loop(group * size, (group + 1) * size, each, carry)

    lax.fori_loop(0, GROUPS, first_sends, 0)
    for group in range(GROUPS):
        load(1, group).start()
    for copy in scalars + sides[1:]:
        copy.wait()
    wave_of = lax.broadcasted_iota(jnp.int32, (waves, LANES), 0)
    angle = jnp.zeros((waves, LANES), jnp.float32)
    for wave in range(waves):
        angle = jnp.where(wave_of == wave, phase[wave], angle)
    turns[0], turns[1] = jnp.cos(angle), jnp.sin(angle)

    gpart[...] = jnp.zeros(gpart.shape, jnp.float32)

    def adjoint_packs(group, carry):
        load(1, group).wait()

        def each(wave, carry):
            pack(1, wave)
            return carry

        return lax.fori_loop(group * size, (group + 1) * size, each, carry)

    lax.fori_loop(0, GROUPS, adjoint_packs, 0)

    eps[rows:] = jnp.ones((TILE, width), jnp.float32)
    for way, at in ((0, rows), (1, total - 2)):
        eps_move(way).wait_recv()
        for part in range(QUARTERS):
            span = slice(part * quarter, (part + 1) * quarter)
            eps[at : at + 2, span] = eps_recv[way, part * 2 : part * 2 + 2]

    row_of = lax.broadcasted_iota(jnp.int32, (total, LANES), 0)

    def spot_of(row):
        away = row - me * rows
        away = jnp.where(away < 0, away + whole, away)
        spot = jnp.where(
            away < rows + REACH, away,
            jnp.where(away >= whole - REACH, away - whole + total, -1),
        )
        return spot

    def turn_of(spot, wave, sign):
        cosine, sine = turns[0, pl.ds(wave, 1)], sign * turns[1, pl.ds(wave, 1)]
        above = (spot >= rows) & (spot < rows + REACH) & at_last
        below = (spot >= rows + REACH) & at_first
        turn_c = jnp.where(above | below, cosine, 1.0)
        turn_s = jnp.where(above, sine, jnp.where(below, -sine, 0.0))
        return turn_c, turn_s

    def unpack(field, wave, sign):
        cosine, sine = turns[0, pl.ds(wave, 1)], sign * turns[1, pl.ds(wave, 1)]
        for way, at in ((0, rows), (1, total - REACH)):
            edge = at_last if way == 0 else at_first
            turn_c = jnp.where(edge, cosine, 1.0)
            turn_s = jnp.where(edge, sine if way == 0 else -sine, 0.0)
            for ct in range(tiles):
                base, place = 2 * REACH * (ct // (tiles // QUARTERS)), col(ct % (tiles // QUARTERS))
                got_re = recv[field, way, wave, base : base + REACH, place]
                got_im = recv[field, way, wave, base + REACH : base + 2 * REACH, place]
                ext[field, wave, 0, at : at + REACH, col(ct)] = turn_c * got_re - turn_s * got_im
                ext[field, wave, 1, at : at + REACH, col(ct)] = turn_s * got_re + turn_c * got_im

    def images(field, group, slot, spot, side_row, with_overlap):
        wave = group * size + slot
        squared_k = wave_k[wave]
        for ct in range(tiles):
            d = 4.0 - squared_k * eps[:, col(ct)]
            diag[:, col(ct)] = d
            inverse[:, col(ct)] = 1.0 / d
        here = row_of == spot
        nears = [
            sideways(lambda ct, c=c: ext[field, wave, c, :, col(ct)], tiles) for c in range(2)
        ]
        for ct in range(tiles):
            rows_in = side_row(ct)
            for c in range(2):
                near = next(nears[c])
                x = ext[field, wave, c, :, col(ct)]
                r = (near + updown(x)) - diag[:, col(ct)] * x
                r = jnp.where(here, r + rows_in[c], r)
                res[c, :, col(ct)] = r
                zed[wave, c, :, col(ct)] = r * inverse[:, col(ct)]
        nears = [sideways(lambda ct, c=c: zed[wave, c, :, col(ct)], tiles) for c in range(2)]
        for ct in range(tiles):
            for c in range(2):
                near = next(nears[c])
                v = res[c, :, col(ct)] - (near + updown(zed[wave, c, :, col(ct)]))
                img[c, :, col(ct)] = v[:rows]
                yed[wave, c, :, col(ct)] = v * inverse[:, col(ct)]
        nears = [
            sideways(lambda ct, c=c: yed[wave, c, 0:rows, col(ct)], tiles) for c in range(2)
        ]
        sums = None
        for ct in range(tiles):
            r, v, w = [], [], []
            for c in range(2):
                near = next(nears[c])
                r.append(res[c, 0:rows, col(ct)])
                v.append(img[c, :, col(ct)])
                w.append(v[c] - (near + updown(yed[wave, c, :, col(ct)])[:rows]))
            found = [
                fold(r[0] * r[0] + r[1] * r[1]), *pair_products(r, v),
                fold(v[0] * v[0] + v[1] * v[1]), *pair_products(w, r), *pair_products(w, v),
                fold(w[0] * w[0] + w[1] * w[1]),
            ]
            sums = found if sums is None else [a + b for a, b in zip(sums, found)]
        for i, value in enumerate(sums):
            parts[group, i, pl.ds(slot, 1)] = jnp.sum(value, axis=0, keepdims=True)
        if with_overlap:
            away = mon_row[wave] - me * rows
            inside = jnp.where((away >= 0) & (away < rows), 1.0, 0.0)
            place = jnp.clip(away, 0, rows - 1)
            held = (
                lambda c: ext[field, wave, c, pl.ds(place, 1)],
                lambda c: zed[wave, c, pl.ds(place, 1)],
                lambda c: yed[wave, c, pl.ds(place, 1)],
            )
            for i, get in enumerate(held):
                sum_re = sum_im = None
                lines = [get(c) for c in range(2)]
                for ct in range(tiles):
                    m = [mon[wave, c : c + 1, col(ct)] for c in range(2)]
                    f = [line[:, col(ct)] for line in lines]
                    new_re = m[0] * f[0] + m[1] * f[1]
                    new_im = m[0] * f[1] - m[1] * f[0]
                    sum_re = new_re if sum_re is None else sum_re + new_re
                    sum_im = new_im if sum_im is None else sum_im + new_im
                parts[group, 9 + 2 * i, pl.ds(slot, 1)] = inside * sum_re
                parts[group, 10 + 2 * i, pl.ds(slot, 1)] = inside * sum_im

    def profile_row(profile, wave, turn, over):
        turn_c, turn_s = turn

        def row(ct):
            p = [profile[wave, c : c + 1, col(ct)] for c in range(2)]
            if over is not None:
                p_re, p_im = times(over, p)
                p = [p_re, -p_im]
            return turn_c * p[0] - turn_s * p[1], turn_s * p[0] + turn_c * p[1]

        return row

    def sum_move(field, group, hop, place):
        return pltpu.make_async_remote_copy(
            src_ref=mine.at[field, group], dst_ref=got.at[field, group, place],
            send_sem=sum_sems.at[0, field, group], recv_sem=sum_sems.at[1, field, group],
            device_id={"gx": lax.rem(me + hop, count)}, device_id_type=pl.DeviceIdType.MESH,
        )

    def all_sums(field, group):
        others = got.at[field, group, pl.ds(0, count - 1)]
        return pltpu.make_async_remote_copy(
            src_ref=others, dst_ref=others,
            send_sem=sum_sems.at[0, field, group], recv_sem=sum_sems.at[1, field, group],
            device_id={"gx": after}, device_id_type=pl.DeviceIdType.MESH,
        )

    slot_of = lax.broadcasted_iota(jnp.int32, (size, LANES), 0)
    lane_of = lax.broadcasted_iota(jnp.int32, (size, LANES), 1)

    def send_sums(field, group):
        used = 15 if field == 0 else 9
        packed = jnp.zeros((size, LANES), jnp.float32)
        for i in range(used):
            own = jnp.sum(parts[group, i], axis=1, keepdims=True)
            packed = jnp.where(lane_of == slot_of * SUMS + i, own, packed)
        line = jnp.sum(packed, axis=0, keepdims=True)
        mine[field, group] = line
        got[field, group, me] = line
        for hop in range(1, count):
            sum_move(field, group, hop, me).start()

    def take_sums(field, group):
        all_sums(field, group).wait_recv()
        line = got[field, group, 0]
        for place in range(1, count):
            line = line + got[field, group, place]
        summed = jnp.broadcast_to(line, (size, LANES))
        for slot in range(1, size):
            turned = pltpu.roll(line, LANES - slot * SUMS, 1)
            summed = jnp.where(slot_of == slot, turned, summed)
        for i, value in enumerate(scalars_of(summed, field == 0)):
            coef[field, group, i] = jnp.broadcast_to(value, (size, LANES))

    def factors(field, group, slot, *kinds):
        return [coef[field, group, i, pl.ds(slot, 1)] for i in kinds]

    def result(field, wave, b, g, span):
        x = [ext[field, wave, c, 0:rows, span] for c in range(2)]
        z = [zed[wave, c, 0:rows, span] for c in range(2)]
        y = [yed[wave, c, 0:rows, span] for c in range(2)]
        bz, gy = times(b, z), times(g, y)
        return x[0] + bz[0] + gy[0], x[1] + bz[1] + gy[1]

    def forward_group(group, carry):
        def each(slot, carry):
            wave = group * size + slot
            for way in range(2):
                halo_move(0, way, wave).wait_recv()
            unpack(0, wave, 1.0)
            spot = spot_of(src_row[wave])
            side = profile_row(src, wave, turn_of(spot, wave, 1.0), None)
            images(0, group, slot, spot, side, True)
            return carry

        lax.fori_loop(0, size, each, 0)
        send_sums(0, group)

        def adjoint_sends(wave, carry):
            for way in range(2):
                halo_move(1, way, wave).start()
            return carry

        @pl.when(group == GROUPS - 3)
        def _():
            lax.fori_loop(0, size, adjoint_sends, 0)

        @pl.when(group == GROUPS - 1)
        def _():
            lax.fori_loop(size, waves, adjoint_sends, 0)

        return carry

    lax.fori_loop(0, GROUPS, forward_group, 0)

    def adjoint_group(group, carry):
        take_sums(0, group)

        def each(slot, carry):
            wave = group * size + slot
            b, g = factors(0, group, slot, 0, 1), factors(0, group, slot, 2, 3)
            over = factors(0, group, slot, 4, 5)
            for ct in range(tiles):
                fwd[wave, 0, :, col(ct)], fwd[wave, 1, :, col(ct)] = result(0, wave, b, g, col(ct))
            for way in range(2):
                halo_move(1, way, wave).wait_recv()
            unpack(1, wave, -1.0)
            spot = spot_of(mon_row[wave])
            side = profile_row(mon, wave, turn_of(spot, wave, -1.0), over)
            images(1, group, slot, spot, side, False)
            return carry

        lax.fori_loop(0, size, each, 0)
        send_sums(1, group)
        return carry

    lax.fori_loop(0, GROUPS, adjoint_group, 0)

    piece = width // depth

    def columns(place):
        return slice(place * piece, (place + 1) * piece)

    def scatter(hop, place):
        return pltpu.make_async_remote_copy(
            src_ref=gpart.at[hop], dst_ref=ggot.at[place],
            send_sem=grad_sems.at[0], recv_sem=grad_sems.at[1],
            device_id={"wa": lax.rem(level + hop, depth)}, device_id_type=pl.DeviceIdType.MESH,
        )

    def gather(hop, place):
        return pltpu.make_async_remote_copy(
            src_ref=gtotal, dst_ref=gspread.at[place],
            send_sem=grad_sems.at[2], recv_sem=grad_sems.at[3],
            device_id={"wa": lax.rem(level + hop, depth)}, device_id_type=pl.DeviceIdType.MESH,
        )

    def all_pieces(held, kind):
        others = held.at[pl.ds(0, depth - 1)]
        return pltpu.make_async_remote_copy(
            src_ref=others, dst_ref=others,
            send_sem=grad_sems.at[2 * kind], recv_sem=grad_sems.at[2 * kind + 1],
            device_id={"wa": lax.rem(level + 1, depth)}, device_id_type=pl.DeviceIdType.MESH,
        )

    def finish(group, hop):
        base = lax.rem(level + hop, depth) * piece
        waves_in = []
        for slot in range(size):
            wave = group * size + slot
            b, g = factors(1, group, slot, 0, 1), factors(1, group, slot, 2, 3)
            waves_in.append((wave, b, g, 2.0 * wave_k[wave]))
        for i in range(piece // LANES):
            span = pl.ds(pl.multiple_of(base + i * LANES, LANES), LANES)
            term = gpart[hop, :, col(i)]
            for wave, b, g, scale in waves_in:
                out_re, out_im = result(1, wave, b, g, span)
                adj[wave, 0, :, span] = out_re
                adj[wave, 1, :, span] = out_im
                fwd_re, fwd_im = fwd[wave, 0, :, span], fwd[wave, 1, :, span]
                term = term + scale * (out_re * fwd_re - out_im * fwd_im)
            gpart[hop, :, col(i)] = term

    def early_group(group, carry):
        take_sums(1, group)
        for hop in range(depth):
            finish(group, hop)
        return carry

    lax.fori_loop(0, GROUPS - 1, early_group, 0)
    for way in range(2):
        eps_move(way).wait_send()
        for field in range(2):
            halos_sent(field, way).wait_send()
    for group in range(GROUPS - 1):
        for field in range(2):
            all_sums(field, group).wait_send()
    all_sums(0, GROUPS - 1).wait_send()

    take_sums(1, GROUPS - 1)
    for hop in sorted(range(1, depth), key=lambda hop: -min(hop, depth - hop)):
        finish(GROUPS - 1, hop)
        scatter(hop, level).start()
    finish(GROUPS - 1, 0)
    ggot[level] = gpart[0]
    all_pieces(ggot, 0).wait_recv()
    summed = ggot[0]
    for place in range(1, depth):
        summed = summed + ggot[place]
    gtotal[...] = summed
    for hop in range(1, depth):
        gather(hop, level).start()
    gspread[level] = summed
    all_sums(1, GROUPS - 1).wait_send()
    all_pieces(ggot, 0).wait_send()
    all_pieces(gspread, 1).wait_recv()
    for place in range(depth):
        grad[:, columns(place)] = mask[:, columns(place)].astype(jnp.float32) * gspread[place]
    all_pieces(gspread, 1).wait_send()


def write_kernel(fwd_in, adj_in, grad_in, fwd, adj, grad, sems):
    waves = fwd_in.shape[0]
    copies = []
    for wave in range(waves):
        copies.append(pltpu.make_async_copy(fwd_in.at[wave], fwd.at[wave], sems.at[0, wave]))
        copies.append(pltpu.make_async_copy(adj_in.at[wave], adj.at[wave], sems.at[1, wave]))
    copies.append(pltpu.make_async_copy(grad_in, grad, sems.at[0, waves]))
    for copy in copies:
        copy.start()
    for copy in copies:
        copy.wait()


def local(
    warm_field,
    warm_adjoint,
    permittivity,
    design_mask,
    source_row,
    monitor_row,
    wavenumber,
    bloch_phase,
    source_profile,
    monitor_profile,
):
    waves, _, rows, width = warm_field.shape
    total = rows + TILE
    count, depth = lax.axis_size("gx"), lax.axis_size("wa")

    vmem = pl.BlockSpec(memory_space=pltpu.VMEM)
    anywhere = pl.BlockSpec(memory_space=pl.ANY)
    f32 = jnp.float32
    piece = (rows, width // depth)
    size = waves // GROUPS
    block = (2 * REACH * QUARTERS, width // QUARTERS)
    fwd, adj, grad = pl.pallas_call(
        functools.partial(step_kernel, count, depth),
        out_shape=(
            pltpu.VMEM(warm_field.shape, f32),
            pltpu.VMEM(warm_field.shape, f32),
            pltpu.VMEM((rows, width), f32),
        ),
        in_specs=[anywhere] * 10,
        out_specs=(vmem, vmem, vmem),
        scratch_shapes=[
            pltpu.VMEM((2, waves, 2, total, width), f32),
            pltpu.VMEM((waves, 2, total, width), f32),
            pltpu.VMEM((waves, 2, total, width), f32),
            pltpu.VMEM((2, 2, waves, *block), f32),
            pltpu.VMEM((2, 2, waves, *block), f32),
            pltpu.VMEM((2, total, width), f32),
            pltpu.VMEM((2, rows, width), f32),
            pltpu.VMEM((total, width), f32),
            pltpu.VMEM((total, width), f32),
            pltpu.VMEM((total, width), f32),
            pltpu.VMEM((2, 2 * QUARTERS, width // QUARTERS), f32),
            pltpu.VMEM((2, 2 * QUARTERS, width // QUARTERS), f32),
            pltpu.VMEM(source_profile.shape, f32),
            pltpu.VMEM(monitor_profile.shape, f32),
            pltpu.VMEM((rows, width), jnp.int32),
            pltpu.SMEM((waves,), f32),
            pltpu.SMEM((waves,), f32),
            pltpu.SMEM((waves,), jnp.int32),
            pltpu.SMEM((waves,), jnp.int32),
            pltpu.VMEM((2, waves, LANES), f32),
            pltpu.VMEM((GROUPS, SUMS, size, LANES), f32),
            pltpu.VMEM((2, GROUPS, 1, LANES), f32),
            pltpu.VMEM((2, GROUPS, count, 1, LANES), f32),
            pltpu.VMEM((2, GROUPS, 6, size, LANES), f32),
            pltpu.VMEM((depth, *piece), f32),
            pltpu.VMEM((depth, *piece), f32),
            pltpu.VMEM(piece, f32),
            pltpu.VMEM((depth, *piece), f32),
            pltpu.SemaphoreType.DMA((2, GROUPS)),
            pltpu.SemaphoreType.DMA((8,)),
            pltpu.SemaphoreType.DMA((2, 2)),
            pltpu.SemaphoreType.DMA((2, 2, waves)),
            pltpu.SemaphoreType.DMA((2, 2)),
            pltpu.SemaphoreType.DMA((2, 2, GROUPS)),
            pltpu.SemaphoreType.DMA((4,)),
        ],
        compiler_params=pltpu.CompilerParams(
            collective_id=0, has_side_effects=True, vmem_limit_bytes=VMEM_LIMIT
        ),
        name="step",
    )(
        bloch_phase, wavenumber, source_row, monitor_row, permittivity, warm_field, warm_adjoint,
        design_mask, source_profile, monitor_profile,
    )
    field_shape = jax.ShapeDtypeStruct(warm_field.shape, f32)
    return pl.pallas_call(
        write_kernel,
        out_shape=(field_shape, field_shape, jax.ShapeDtypeStruct((rows, width), f32)),
        in_specs=[vmem, vmem, vmem],
        out_specs=(anywhere, anywhere, anywhere),
        scratch_shapes=[pltpu.SemaphoreType.DMA((2, waves + 1))],
        compiler_params=pltpu.CompilerParams(vmem_limit_bytes=1024 * 1024),
        name="write_out",
    )(fwd, adj, grad)


def solution(mesh):
    placed = (
        P("wa", None, "gx", None),
        P("wa", None, "gx", None),
        P("gx", None),
        P("gx", None),
        P("wa"),
        P("wa"),
        P("wa"),
        P("wa"),
        P("wa", None, None),
        P("wa", None, None),
    )
    return jax.shard_map(
        local,
        mesh=mesh,
        in_specs=placed,
        out_specs=(P("wa", None, "gx", None), P("wa", None, "gx", None), P("gx", None)),
        check_vma=False,
    )
```

```python
import functools

import jax
import jax.numpy as jnp
from jax import lax
from jax.experimental import pallas as pl
from jax.experimental.pallas import tpu as pltpu
from jax.sharding import PartitionSpec as P

floor_share = 0.5
REACH = 3
TILE = 8
LANES = 128
QUARTERS = 4
SUMS = 16
GROUPS = 4
VMEM_LIMIT = 50000 * 1024


def col(tile):
    return slice(tile * LANES, (tile + 1) * LANES)


def sideways(load, tiles):
    tile = load(0)
    lane = lax.broadcasted_iota(jnp.int32, tile.shape, 1)
    at_right, at_left = lane == LANES - 1, lane == 0
    after, before = pltpu.roll(tile, LANES - 1, 1), pltpu.roll(tile, 1, 1)
    carried = jnp.zeros_like(tile)
    for ct in range(tiles):
        if ct + 1 < tiles:
            ahead = load(ct + 1)
            next_after, next_before = pltpu.roll(ahead, LANES - 1, 1), pltpu.roll(ahead, 1, 1)
        else:
            ahead, next_after, next_before = None, jnp.zeros_like(tile), None
        near = jnp.where(at_right, next_after, after) + jnp.where(at_left, carried, before)
        yield near
        carried, tile, after, before = before, ahead, next_after, next_before


def updown(tile):
    total = tile.shape[0]
    return pltpu.roll(tile, total - 1, 0) + pltpu.roll(tile, 1, 0)


def fold(cells):
    acc = cells[:TILE]
    for start in range(TILE, cells.shape[0], TILE):
        acc = acc + cells[start : start + TILE]
    return acc


def pair_products(a, b):
    return fold(a[0] * b[0] + a[1] * b[1]), fold(a[0] * b[1] - a[1] * b[0])


def times(a, b):
    return a[0] * b[0] - a[1] * b[1], a[0] * b[1] + a[1] * b[0]


def scalars_of(total, with_overlap):
    q = [total[:, i : i + 1] for i in range(SUMS)]
    res_norm, rv_re, rv_im, image_sq, wr_re, wr_im, wv_re, wv_im, twice_sq = q[:9]
    half = floor_share * res_norm
    bounded = jnp.maximum(rv_re * rv_re + rv_im * rv_im, half * half)
    step_re = res_norm * rv_re / bounded
    step_im = -res_norm * rv_im / bounded
    step_sq = step_re * step_re + step_im * step_im
    ts_re = rv_re - step_re * image_sq - (step_re * wr_re + step_im * wr_im) + step_sq * wv_re
    ts_im = -rv_im - step_im * image_sq - (step_re * wr_im - step_im * wr_re) + step_sq * wv_im
    tt_sum = image_sq - 2.0 * (step_re * wv_re + step_im * wv_im) + step_sq * twice_sq
    omega_re = ts_re / tt_sum
    omega_im = ts_im / tt_sum
    both_re, both_im = times((step_re, step_im), (omega_re, omega_im))
    found = [step_re + omega_re, step_im + omega_im, -both_re, -both_im]
    if with_overlap:
        mx_re, mx_im, mz_re, mz_im, my_re, my_im = q[9:15]
        for_z = times(found[0:2], (mz_re, mz_im))
        for_y = times(found[2:4], (my_re, my_im))
        found.append(mx_re + for_z[0] + for_y[0])
        found.append(mx_im + for_z[1] + for_y[1])
    return found


def step_kernel(
    count, depth,
    phase_hbm, wave_hbm, src_row_hbm, mon_row_hbm, eps_hbm, field_hbm, adjoint_hbm, mask_hbm, src_hbm, mon_hbm,
    fwd, adj, grad,
    ext, zed, yed, send, recv, res, img, diag, inverse, eps, eps_send, eps_recv, src, mon, mask,
    phase, wave_k, src_row, mon_row, turns, parts, mine, got, coef, gpart, ggot, gtotal, gspread,
    load_sem, side_sem, sent_sem, halo_sem, eps_sems, sum_sems, grad_sems,
):
    waves, _, rows, width = field_hbm.shape
    total = rows + TILE
    tiles = width // LANES
    quarter = width // QUARTERS
    size = waves // GROUPS
    whole = rows * count
    me = lax.axis_index("gx")
    level = lax.axis_index("wa")
    before, after = lax.rem(me - 1 + count, count), lax.rem(me + 1, count)
    at_first, at_last = me == 0, me == count - 1

    fields = (field_hbm, adjoint_hbm)

    def load(field, group):
        members = pl.ds(group * size, size)
        return pltpu.make_async_copy(
            fields[field].at[members], ext.at[field, members, :, pl.ds(0, rows)],
            load_sem.at[field, group],
        )

    sides = [
        pltpu.make_async_copy(eps_hbm, eps.at[pl.ds(0, rows)], side_sem.at[0]),
        pltpu.make_async_copy(src_hbm, src, side_sem.at[1]),
        pltpu.make_async_copy(mon_hbm, mon, side_sem.at[2]),
        pltpu.make_async_copy(mask_hbm, mask, side_sem.at[3]),
    ]
    scalars = [
        pltpu.make_async_copy(phase_hbm, phase, side_sem.at[4]),
        pltpu.make_async_copy(wave_hbm, wave_k, side_sem.at[5]),
        pltpu.make_async_copy(src_row_hbm, src_row, side_sem.at[6]),
        pltpu.make_async_copy(mon_row_hbm, mon_row, side_sem.at[7]),
    ]
    barrier = pltpu.get_barrier_semaphore()
    for axis, extent, own in (("wa", depth, level), ("gx", count, me)):
        for hop in range(1, extent):
            pl.semaphore_signal(
                barrier, inc=1, device_id={axis: lax.rem(own + hop, extent)},
                device_id_type=pl.DeviceIdType.MESH,
            )
    sides[0].start()
    for group in range(GROUPS):
        load(0, group).start()
    for copy in scalars + sides[1:]:
        copy.start()

    sides[0].wait()
    for way, low in ((0, 0), (1, rows - 2)):
        for part in range(QUARTERS):
            span = slice(part * quarter, (part + 1) * quarter)
            eps_send[way, part * 2 : part * 2 + 2] = eps[low : low + 2, span]

    def neighbour(way):
        return {"gx": before if way == 0 else after}

    def eps_move(way):
        return pltpu.make_async_remote_copy(
            src_ref=eps_send.at[way], dst_ref=eps_recv.at[way],
            send_sem=eps_sems.at[0, way], recv_sem=eps_sems.at[1, way],
            device_id=neighbour(way), device_id_type=pl.DeviceIdType.MESH,
        )

    def halo_move(field, way, wave):
        return pltpu.make_async_remote_copy(
            src_ref=send.at[field, way, wave], dst_ref=recv.at[field, way, wave],
            send_sem=sent_sem.at[field, way], recv_sem=halo_sem.at[field, way, wave],
            device_id=neighbour(way), device_id_type=pl.DeviceIdType.MESH,
        )

    def halos_sent(field, way):
        return pltpu.make_async_remote_copy(
            src_ref=send.at[field, way], dst_ref=recv.at[field, way],
            send_sem=sent_sem.at[field, way], recv_sem=halo_sem.at[field, way, 0],
            device_id=neighbour(way), device_id_type=pl.DeviceIdType.MESH,
        )

    def pack(field, wave):
        for way, low in ((0, 0), (1, rows - REACH)):
            for c in range(2):
                for part in range(QUARTERS):
                    span = slice(part * quarter, (part + 1) * quarter)
                    at = part * 2 * REACH + c * REACH
                    send[field, way, wave, at : at + REACH] = ext[
                        field, wave, c, low : low + REACH, span
                    ]

    pl.semaphore_wait(barrier, count - 1 + depth - 1)
    for way in range(2):
        eps_move(way).start()

    def first_sends(group, carry):
        load(0, group).wait()

        def each(wave, carry):
            pack(0, wave)
            for way in range(2):
                halo_move(0, way, wave).start()
            return carry

        return lax.fori_loop(group * size, (group + 1) * size, each, carry)

    lax.fori_loop(0, GROUPS, first_sends, 0)
    for group in range(GROUPS):
        load(1, group).start()
    for copy in scalars + sides[1:]:
        copy.wait()
    wave_of = lax.broadcasted_iota(jnp.int32, (waves, LANES), 0)
    angle = jnp.zeros((waves, LANES), jnp.float32)
    for wave in range(waves):
        angle = jnp.where(wave_of == wave, phase[wave], angle)
    turns[0], turns[1] = jnp.cos(angle), jnp.sin(angle)

    gpart[...] = jnp.zeros(gpart.shape, jnp.float32)

    def adjoint_packs(group, carry):
        load(1, group).wait()

        def each(wave, carry):
            pack(1, wave)
            return carry

        return lax.fori_loop(group * size, (group + 1) * size, each, carry)

    lax.fori_loop(0, GROUPS, adjoint_packs, 0)

    eps[rows:] = jnp.ones((TILE, width), jnp.float32)
    for way, at in ((0, rows), (1, total - 2)):
        eps_move(way).wait_recv()
        for part in range(QUARTERS):
            span = slice(part * quarter, (part + 1) * quarter)
            eps[at : at + 2, span] = eps_recv[way, part * 2 : part * 2 + 2]

    row_of = lax.broadcasted_iota(jnp.int32, (total, LANES), 0)

    def spot_of(row):
        away = row - me * rows
        away = jnp.where(away < 0, away + whole, away)
        spot = jnp.where(
            away < rows + REACH, away,
            jnp.where(away >= whole - REACH, away - whole + total, -1),
        )
        return spot

    def turn_of(spot, wave, sign):
        cosine, sine = turns[0, pl.ds(wave, 1)], sign * turns[1, pl.ds(wave, 1)]
        above = (spot >= rows) & (spot < rows + REACH) & at_last
        below = (spot >= rows + REACH) & at_first
        turn_c = jnp.where(above | below, cosine, 1.0)
        turn_s = jnp.where(above, sine, jnp.where(below, -sine, 0.0))
        return turn_c, turn_s

    def unpack(field, wave, sign):
        cosine, sine = turns[0, pl.ds(wave, 1)], sign * turns[1, pl.ds(wave, 1)]
        for way, at in ((0, rows), (1, total - REACH)):
            edge = at_last if way == 0 else at_first
            turn_c = jnp.where(edge, cosine, 1.0)
            turn_s = jnp.where(edge, sine if way == 0 else -sine, 0.0)
            for ct in range(tiles):
                base, place = 2 * REACH * (ct // (tiles // QUARTERS)), col(ct % (tiles // QUARTERS))
                got_re = recv[field, way, wave, base : base + REACH, place]
                got_im = recv[field, way, wave, base + REACH : base + 2 * REACH, place]
                ext[field, wave, 0, at : at + REACH, col(ct)] = turn_c * got_re - turn_s * got_im
                ext[field, wave, 1, at : at + REACH, col(ct)] = turn_s * got_re + turn_c * got_im

    def images(field, group, slot, spot, side_row, with_overlap):
        wave = group * size + slot
        squared_k = wave_k[wave]
        for ct in range(tiles):
            d = 4.0 - squared_k * eps[:, col(ct)]
            diag[:, col(ct)] = d
            inverse[:, col(ct)] = 1.0 / d
        here = row_of == spot
        nears = [
            sideways(lambda ct, c=c: ext[field, wave, c, :, col(ct)], tiles) for c in range(2)
        ]
        for ct in range(tiles):
            rows_in = side_row(ct)
            for c in range(2):
                near = next(nears[c])
                x = ext[field, wave, c, :, col(ct)]
                r = (near + updown(x)) - diag[:, col(ct)] * x
                r = jnp.where(here, r + rows_in[c], r)
                res[c, :, col(ct)] = r
                zed[wave, c, :, col(ct)] = r * inverse[:, col(ct)]
        nears = [sideways(lambda ct, c=c: zed[wave, c, :, col(ct)], tiles) for c in range(2)]
        for ct in range(tiles):
            for c in range(2):
                near = next(nears[c])
                v = res[c, :, col(ct)] - (near + updown(zed[wave, c, :, col(ct)]))
                img[c, :, col(ct)] = v[:rows]
                yed[wave, c, :, col(ct)] = v * inverse[:, col(ct)]
        nears = [
            sideways(lambda ct, c=c: yed[wave, c, 0:rows, col(ct)], tiles) for c in range(2)
        ]
        sums = None
        for ct in range(tiles):
            r, v, w = [], [], []
            for c in range(2):
                near = next(nears[c])
                r.append(res[c, 0:rows, col(ct)])
                v.append(img[c, :, col(ct)])
                w.append(v[c] - (near + updown(yed[wave, c, :, col(ct)])[:rows]))
            found = [
                fold(r[0] * r[0] + r[1] * r[1]), *pair_products(r, v),
                fold(v[0] * v[0] + v[1] * v[1]), *pair_products(w, r), *pair_products(w, v),
                fold(w[0] * w[0] + w[1] * w[1]),
            ]
            sums = found if sums is None else [a + b for a, b in zip(sums, found)]
        for i, value in enumerate(sums):
            parts[group, i, pl.ds(slot, 1)] = jnp.sum(value, axis=0, keepdims=True)
        if with_overlap:
            away = mon_row[wave] - me * rows
            inside = jnp.where((away >= 0) & (away < rows), 1.0, 0.0)
            place = jnp.clip(away, 0, rows - 1)
            held = (
                lambda c: ext[field, wave, c, pl.ds(place, 1)],
                lambda c: zed[wave, c, pl.ds(place, 1)],
                lambda c: yed[wave, c, pl.ds(place, 1)],
            )
            for i, get in enumerate(held):
                sum_re = sum_im = None
                lines = [get(c) for c in range(2)]
                for ct in range(tiles):
                    m = [mon[wave, c : c + 1, col(ct)] for c in range(2)]
                    f = [line[:, col(ct)] for line in lines]
                    new_re = m[0] * f[0] + m[1] * f[1]
                    new_im = m[0] * f[1] - m[1] * f[0]
                    sum_re = new_re if sum_re is None else sum_re + new_re
                    sum_im = new_im if sum_im is None else sum_im + new_im
                parts[group, 9 + 2 * i, pl.ds(slot, 1)] = inside * sum_re
                parts[group, 10 + 2 * i, pl.ds(slot, 1)] = inside * sum_im

    def profile_row(profile, wave, turn, over):
        turn_c, turn_s = turn

        def row(ct):
            p = [profile[wave, c : c + 1, col(ct)] for c in range(2)]
            if over is not None:
                p_re, p_im = times(over, p)
                p = [p_re, -p_im]
            return turn_c * p[0] - turn_s * p[1], turn_s * p[0] + turn_c * p[1]

        return row

    def sum_move(field, group, hop, place):
        return pltpu.make_async_remote_copy(
            src_ref=mine.at[field, group], dst_ref=got.at[field, group, place],
            send_sem=sum_sems.at[0, field, group], recv_sem=sum_sems.at[1, field, group],
            device_id={"gx": lax.rem(me + hop, count)}, device_id_type=pl.DeviceIdType.MESH,
        )

    def all_sums(field, group):
        others = got.at[field, group, pl.ds(0, count - 1)]
        return pltpu.make_async_remote_copy(
            src_ref=others, dst_ref=others,
            send_sem=sum_sems.at[0, field, group], recv_sem=sum_sems.at[1, field, group],
            device_id={"gx": after}, device_id_type=pl.DeviceIdType.MESH,
        )

    slot_of = lax.broadcasted_iota(jnp.int32, (size, LANES), 0)
    lane_of = lax.broadcasted_iota(jnp.int32, (size, LANES), 1)

    def send_sums(field, group):
        used = 15 if field == 0 else 9
        packed = jnp.zeros((size, LANES), jnp.float32)
        for i in range(used):
            own = jnp.sum(parts[group, i], axis=1, keepdims=True)
            packed = jnp.where(lane_of == slot_of * SUMS + i, own, packed)
        line = jnp.sum(packed, axis=0, keepdims=True)
        mine[field, group] = line
        got[field, group, me] = line
        for hop in range(1, count):
            sum_move(field, group, hop, me).start()

    def step_factors(field, group):
        line = got[field, group, 0]
        for place in range(1, count):
            line = line + got[field, group, place]
        summed = jnp.broadcast_to(line, (size, LANES))
        for slot in range(1, size):
            turned = pltpu.roll(line, LANES - slot * SUMS, 1)
            summed = jnp.where(slot_of == slot, turned, summed)
        for i, value in enumerate(scalars_of(summed, field == 0)):
            coef[field, group, i] = jnp.broadcast_to(value, (size, LANES))

    def take_sums(field, group):
        all_sums(field, group).wait_recv()
        step_factors(field, group)

    def factors(field, group, slot, *kinds):
        return [coef[field, group, i, pl.ds(slot, 1)] for i in kinds]

    def result(field, wave, b, g, span):
        x = [ext[field, wave, c, 0:rows, span] for c in range(2)]
        z = [zed[wave, c, 0:rows, span] for c in range(2)]
        y = [yed[wave, c, 0:rows, span] for c in range(2)]
        bz, gy = times(b, z), times(g, y)
        return x[0] + bz[0] + gy[0], x[1] + bz[1] + gy[1]

    def forward_group(group, carry):
        def each(slot, carry):
            wave = group * size + slot
            for way in range(2):
                halo_move(0, way, wave).wait_recv()
            unpack(0, wave, 1.0)
            spot = spot_of(src_row[wave])
            side = profile_row(src, wave, turn_of(spot, wave, 1.0), None)
            images(0, group, slot, spot, side, True)
            return carry

        lax.fori_loop(0, size, each, 0)
        send_sums(0, group)

        def adjoint_sends(wave, carry):
            for way in range(2):
                halo_move(1, way, wave).start()
            return carry

        @pl.when(group == GROUPS - 3)
        def _():
            lax.fori_loop(0, size, adjoint_sends, 0)

        @pl.when(group == GROUPS - 1)
        def _():
            lax.fori_loop(size, waves, adjoint_sends, 0)

        return carry

    lax.fori_loop(0, GROUPS, forward_group, 0)

    def adjoint_group(group, carry):
        take_sums(0, group)

        def each(slot, carry):
            wave = group * size + slot
            b, g = factors(0, group, slot, 0, 1), factors(0, group, slot, 2, 3)
            over = factors(0, group, slot, 4, 5)
            for ct in range(tiles):
                fwd[wave, 0, :, col(ct)], fwd[wave, 1, :, col(ct)] = result(0, wave, b, g, col(ct))
            for way in range(2):
                halo_move(1, way, wave).wait_recv()
            unpack(1, wave, -1.0)
            spot = spot_of(mon_row[wave])
            side = profile_row(mon, wave, turn_of(spot, wave, -1.0), over)
            images(1, group, slot, spot, side, False)
            return carry

        lax.fori_loop(0, size, each, 0)
        send_sums(1, group)
        return carry

    lax.fori_loop(0, GROUPS, adjoint_group, 0)

    piece = width // depth

    def columns(place):
        return slice(place * piece, (place + 1) * piece)

    def scatter(hop, place):
        return pltpu.make_async_remote_copy(
            src_ref=gpart.at[hop], dst_ref=ggot.at[place],
            send_sem=grad_sems.at[0], recv_sem=grad_sems.at[1],
            device_id={"wa": lax.rem(level + hop, depth)}, device_id_type=pl.DeviceIdType.MESH,
        )

    def gather(hop, place):
        return pltpu.make_async_remote_copy(
            src_ref=gtotal, dst_ref=gspread.at[place],
            send_sem=grad_sems.at[2], recv_sem=grad_sems.at[3],
            device_id={"wa": lax.rem(level + hop, depth)}, device_id_type=pl.DeviceIdType.MESH,
        )

    def all_pieces(held, kind):
        others = held.at[pl.ds(0, depth - 1)]
        return pltpu.make_async_remote_copy(
            src_ref=others, dst_ref=others,
            send_sem=grad_sems.at[2 * kind], recv_sem=grad_sems.at[2 * kind + 1],
            device_id={"wa": lax.rem(level + 1, depth)}, device_id_type=pl.DeviceIdType.MESH,
        )

    def finish(group, hop):
        base = lax.rem(level + hop, depth) * piece
        waves_in = []
        for slot in range(size):
            wave = group * size + slot
            b, g = factors(1, group, slot, 0, 1), factors(1, group, slot, 2, 3)
            waves_in.append((wave, b, g, 2.0 * wave_k[wave]))
        for i in range(piece // LANES):
            span = pl.ds(pl.multiple_of(base + i * LANES, LANES), LANES)
            term = gpart[hop, :, col(i)]
            for wave, b, g, scale in waves_in:
                out_re, out_im = result(1, wave, b, g, span)
                adj[wave, 0, :, span] = out_re
                adj[wave, 1, :, span] = out_im
                fwd_re, fwd_im = fwd[wave, 0, :, span], fwd[wave, 1, :, span]
                term = term + scale * (out_re * fwd_re - out_im * fwd_im)
            gpart[hop, :, col(i)] = term

    def early_group(group, carry):
        for hop in range(depth):
            finish(group, hop)
        return carry

    for group in range(GROUPS - 1):
        all_sums(1, group).wait_recv()
    for group in range(GROUPS - 1):
        step_factors(1, group)
    lax.fori_loop(0, GROUPS - 1, early_group, 0)
    for way in range(2):
        eps_move(way).wait_send()
        for field in range(2):
            halos_sent(field, way).wait_send()
    for group in range(GROUPS - 1):
        for field in range(2):
            all_sums(field, group).wait_send()
    all_sums(0, GROUPS - 1).wait_send()

    take_sums(1, GROUPS - 1)
    for hop in sorted(range(1, depth), key=lambda hop: -min(hop, depth - hop)):
        finish(GROUPS - 1, hop)
        scatter(hop, level).start()
    finish(GROUPS - 1, 0)
    ggot[level] = gpart[0]
    all_pieces(ggot, 0).wait_recv()
    summed = ggot[0]
    for place in range(1, depth):
        summed = summed + ggot[place]
    gtotal[...] = summed
    for hop in range(1, depth):
        gather(hop, level).start()
    gspread[level] = summed
    all_sums(1, GROUPS - 1).wait_send()
    all_pieces(ggot, 0).wait_send()
    all_pieces(gspread, 1).wait_recv()
    for place in range(depth):
        grad[:, columns(place)] = mask[:, columns(place)].astype(jnp.float32) * gspread[place]
    all_pieces(gspread, 1).wait_send()


def write_kernel(fwd_in, adj_in, grad_in, fwd, adj, grad, sems):
    waves = fwd_in.shape[0]
    copies = []
    for wave in range(waves):
        copies.append(pltpu.make_async_copy(fwd_in.at[wave], fwd.at[wave], sems.at[0, wave]))
        copies.append(pltpu.make_async_copy(adj_in.at[wave], adj.at[wave], sems.at[1, wave]))
    copies.append(pltpu.make_async_copy(grad_in, grad, sems.at[0, waves]))
    for copy in copies:
        copy.start()
    for copy in copies:
        copy.wait()


def local(
    warm_field,
    warm_adjoint,
    permittivity,
    design_mask,
    source_row,
    monitor_row,
    wavenumber,
    bloch_phase,
    source_profile,
    monitor_profile,
):
    waves, _, rows, width = warm_field.shape
    total = rows + TILE
    count, depth = lax.axis_size("gx"), lax.axis_size("wa")

    vmem = pl.BlockSpec(memory_space=pltpu.VMEM)
    anywhere = pl.BlockSpec(memory_space=pl.ANY)
    f32 = jnp.float32
    piece = (rows, width // depth)
    size = waves // GROUPS
    block = (2 * REACH * QUARTERS, width // QUARTERS)
    fwd, adj, grad = pl.pallas_call(
        functools.partial(step_kernel, count, depth),
        out_shape=(
            pltpu.VMEM(warm_field.shape, f32),
            pltpu.VMEM(warm_field.shape, f32),
            pltpu.VMEM((rows, width), f32),
        ),
        in_specs=[anywhere] * 10,
        out_specs=(vmem, vmem, vmem),
        scratch_shapes=[
            pltpu.VMEM((2, waves, 2, total, width), f32),
            pltpu.VMEM((waves, 2, total, width), f32),
            pltpu.VMEM((waves, 2, total, width), f32),
            pltpu.VMEM((2, 2, waves, *block), f32),
            pltpu.VMEM((2, 2, waves, *block), f32),
            pltpu.VMEM((2, total, width), f32),
            pltpu.VMEM((2, rows, width), f32),
            pltpu.VMEM((total, width), f32),
            pltpu.VMEM((total, width), f32),
            pltpu.VMEM((total, width), f32),
            pltpu.VMEM((2, 2 * QUARTERS, width // QUARTERS), f32),
            pltpu.VMEM((2, 2 * QUARTERS, width // QUARTERS), f32),
            pltpu.VMEM(source_profile.shape, f32),
            pltpu.VMEM(monitor_profile.shape, f32),
            pltpu.VMEM((rows, width), jnp.int32),
            pltpu.SMEM((waves,), f32),
            pltpu.SMEM((waves,), f32),
            pltpu.SMEM((waves,), jnp.int32),
            pltpu.SMEM((waves,), jnp.int32),
            pltpu.VMEM((2, waves, LANES), f32),
            pltpu.VMEM((GROUPS, SUMS, size, LANES), f32),
            pltpu.VMEM((2, GROUPS, 1, LANES), f32),
            pltpu.VMEM((2, GROUPS, count, 1, LANES), f32),
            pltpu.VMEM((2, GROUPS, 6, size, LANES), f32),
            pltpu.VMEM((depth, *piece), f32),
            pltpu.VMEM((depth, *piece), f32),
            pltpu.VMEM(piece, f32),
            pltpu.VMEM((depth, *piece), f32),
            pltpu.SemaphoreType.DMA((2, GROUPS)),
            pltpu.SemaphoreType.DMA((8,)),
            pltpu.SemaphoreType.DMA((2, 2)),
            pltpu.SemaphoreType.DMA((2, 2, waves)),
            pltpu.SemaphoreType.DMA((2, 2)),
            pltpu.SemaphoreType.DMA((2, 2, GROUPS)),
            pltpu.SemaphoreType.DMA((4,)),
        ],
        compiler_params=pltpu.CompilerParams(
            collective_id=0, has_side_effects=True, vmem_limit_bytes=VMEM_LIMIT
        ),
        name="step",
    )(
        bloch_phase, wavenumber, source_row, monitor_row, permittivity, warm_field, warm_adjoint,
        design_mask, source_profile, monitor_profile,
    )
    field_shape = jax.ShapeDtypeStruct(warm_field.shape, f32)
    return pl.pallas_call(
        write_kernel,
        out_shape=(field_shape, field_shape, jax.ShapeDtypeStruct((rows, width), f32)),
        in_specs=[vmem, vmem, vmem],
        out_specs=(anywhere, anywhere, anywhere),
        scratch_shapes=[pltpu.SemaphoreType.DMA((2, waves + 1))],
        compiler_params=pltpu.CompilerParams(vmem_limit_bytes=1024 * 1024),
        name="write_out",
    )(fwd, adj, grad)


def solution(mesh):
    placed = (
        P("wa", None, "gx", None),
        P("wa", None, "gx", None),
        P("gx", None),
        P("gx", None),
        P("wa"),
        P("wa"),
        P("wa"),
        P("wa"),
        P("wa", None, None),
        P("wa", None, None),
    )
    return jax.shard_map(
        local,
        mesh=mesh,
        in_specs=placed,
        out_specs=(P("wa", None, "gx", None), P("wa", None, "gx", None), P("gx", None)),
        check_vma=False,
    )
```
